128 devices in a mesh: gx: 8 (over z, core), yz: 16 (over y, x).
Axes of the slice: x: 4, y: 4, z: 4, core: 2. Of those that a mesh axis runs over, the one named last changes fastest.
Arguments:
- brick_ids: int32 [16384, 1], P(('gx', 'yz')), may hold values from 0 to 127; in each aligned block of 128 rows (0 to 127, 128 to 255, ...) at most 2 rows name the same one
- voxel_offset: int32 [16384, 256], P(('gx', 'yz')), may hold values from 0 to 4095
- fractions: float32 [16384, 3, 256], P(('gx', 'yz')), may hold values from 0 to 1
- normals: float32 [16384, 3, 256], P(('gx', 'yz')), may hold values from -6 to 6
- point_weight: float32 [16384, 256], P(('gx', 'yz')), may hold values from 0.1 to 10
- tile_count: int32 [128], P(('gx', 'yz')), may hold values from 96 to 128, as said below
Outputs:
- rhs: float32 [32, 128, 128], P('gx', 'yz')
- screen: float32 [32, 128, 128], P('gx', 'yz')
The draws below stay inside these ranges and needn't reach their ends.
Inputs may be any that keep to these rules, and one draw needn't show every extreme that they name: `brick_ids`: brick b belongs to index b // 16 of gx and b % 16 of yz. Among the 128 tile slots of one device no brick is named more than 2 times. `tile_count`: some device has all its slots valid in every draw.
All inputs are finite; a program needn't handle non-finite values.
Results may differ from the reference program's by a relative error of at most 0.0039.
Values sent between devices are 32-bit elements; how exact they have to be, the bound alone decides.
No kernel may reach another device: no remote copies, remote signals or barrier semaphores. Data moves between devices by JAX's collectives and lax.ppermute only.
A program may use at most 64 MiB of HBM per device.

```python
import math
import jax
import jax.numpy as jnp
import numpy as np
from jax import lax

BX = 4
BY = 8
BZ = 128
TILE = 256
TILES_DEV = 128
CAP = 2
TILES = 16384
NX = 32
NY = 128
NZ = 128
N_YZ = 16
DEVICES = 128


def draw_tile_count(key, part):
    first = jax.random.fold_in(key, 11)
    second = jax.random.fold_in(key, 23)
    counts = jax.random.randint(first, (DEVICES,), max(1, 3 * TILES_DEV // 4), TILES_DEV + 1)
    filled = jax.random.randint(second, (), 0, DEVICES)
    return counts.at[filled].set(TILES_DEV).astype(jnp.int32)


def place_ends(entries, stream_key, least, high):
    longest = entries.shape.index(max(entries.shape))
    spots = []
    for shift in (0, 1):
        where = [jax.random.randint(jax.random.fold_in(stream_key, axis), (), 0, length) for axis, length in enumerate(entries.shape)]
        where[longest] = (where[longest] + shift) % entries.shape[longest]
        spots.append(tuple(where))
    return entries.at[spots[0]].set(least).at[spots[1]].set(high)


def level_of(rng, shape, cuts, low, top_value):
    factor_of = 1.0
    for dim, blocks in cuts:
        draws = jax.random.uniform(jax.random.fold_in(jax.random.fold_in(rng, 6), dim), (blocks,), jnp.float32, low / len(cuts), top_value / len(cuts))
        factor_of = factor_of * jnp.repeat(jnp.exp(draws), shape[dim] // blocks).reshape((-1,) + (1,) * (len(shape) - 1 - dim))
    return factor_of


def deal_out(key, own, number, rows, count, top, reach, slope):
    sequence = jax.random.permutation(key, count)
    crowded, usual = shares(count, rows * top, reach, slope, True), shares(count, rows * top, reach, slope, False)
    places = jnp.arange(count)

    def named(tallies, turn):
        used = int((tallies > 0).sum())
        fixed = max(1, used // 4)
        shifted = fixed + (places - fixed + turn * (used - fixed)) % max(1, count - fixed)
        return jnp.zeros((count,), jnp.int32).at[sequence[jnp.where(places < fixed, places, shifted)]].set(jnp.asarray(tallies, jnp.int32))

    tallies = jnp.where(number % 4 == 0, named(crowded, number // 4), named(usual, number - number // 4 - 1))
    mixed = jax.random.permutation(jax.random.fold_in(own, 3), count)
    donor, sink = mixed[0:count // 2 * 2:2], mixed[1:count // 2 * 2:2]
    room = jnp.minimum(tallies[donor] - 1, reach - tallies[sink]) // 2
    room = jnp.where((donor == sequence[0]) | (sink == sequence[0]) | (tallies[sink] == 0), 0, jnp.maximum(room, 0))
    shifted = jax.random.randint(jax.random.fold_in(own, 4), (count // 2,), 0, 1 << 20) % (room + 1)
    tallies = tallies.at[donor].add(-shifted).at[sink].add(shifted)
    labels = jnp.searchsorted(jnp.cumsum(tallies), jnp.arange(rows * top), side="right").astype(jnp.int32)
    grid = labels.reshape(top, rows).T
    grid = grid[jax.random.permutation(jax.random.fold_in(own, 1), rows)]
    turn = jax.random.randint(jax.random.fold_in(own, 2), (rows, 1), 0, top)
    return jnp.take_along_axis(grid, (jnp.arange(top)[None, :] + turn) % top, axis=1)


def shares(amount, total, bound, skew, full):
    weights = [(1 << 20) // math.isqrt(standing ** skew) + 1 for standing in range(1, amount + 1)]
    largest = bound if full else min(bound, max(-(-total // amount), total * weights[0] // sum(weights)))
    least = 1 if total - largest >= amount - 1 else 0
    given, spare = [largest] + [least] * (amount - 1), total - largest - least * (amount - 1)
    while spare > 0:
        movable = [i for i in range(1, amount) if given[i] < largest] or [i for i in range(1, amount) if given[i] < bound]
        whole, budget = sum([weights[i] for i in movable]), spare
        for i in movable:
            more = min(bound - given[i], max(1, budget * weights[i] // whole), spare)
            given[i] = given[i] + more
            spare = spare - more
    return np.array(given)


def bell_draw(rng, shape, scale, most, cuts=(), kind=jnp.bfloat16):
    result = jax.random.normal(rng, shape, jnp.float32) * scale
    if len(cuts) > 0:
        result = level_of(rng, shape, cuts, -0.22, 0.18) * result
    return jnp.clip(result, min=-most, max=most).astype(kind)


def setup_inputs(seed: int = 0) -> dict:
    arg_keys = jax.random.split(jax.random.key(seed), 7)
    brick_ids_keys = jax.random.split(jax.random.fold_in(arg_keys[0], 1), TILES // TILES_DEV)
    brick_ids_turns = jax.random.permutation(jax.random.fold_in(arg_keys[0], 3), TILES // TILES_DEV)
    brick_ids = jax.vmap(lambda own, number: deal_out(jax.random.fold_in(arg_keys[0], 2), own, number, TILES_DEV, DEVICES, 1, CAP, 2))(brick_ids_keys, brick_ids_turns).reshape((TILES, 1))
    voxel_offset = place_ends(jax.random.randint(arg_keys[1], (TILES, TILE), 0, BX * BY * BZ), jax.random.fold_in(arg_keys[1], 1), 0, (BX * BY * BZ) - 1).astype(jnp.int32)
    fractions = jnp.clip(1.0 * jax.random.uniform(arg_keys[2], (TILES, 3, TILE), jnp.float32) ** level_of(arg_keys[2], (TILES, 3, TILE), ((0, 128),), -0.2, 0.2), 0.0, 1.0)
    normals = bell_draw(arg_keys[3], (TILES, 3, TILE), 1.0, 6.0, ((0, 128),), jnp.float32)
    point_weight = jnp.clip(jnp.exp(math.log(10.0) - 4.6051702 * jax.random.uniform(arg_keys[4], (TILES, TILE), jnp.float32) ** level_of(arg_keys[4], (TILES, TILE), ((0, 128),), -0.2, 0.2)), 0.1, 10.0)
    tile_count = draw_tile_count(jax.random.fold_in(arg_keys[6], 71), 0)
    return dict(brick_ids=brick_ids, voxel_offset=voxel_offset, fractions=fractions, normals=normals, point_weight=point_weight, tile_count=tile_count)


def spline(frac):
    weights = jnp.stack([0.5 * (1.0 - frac) ** 2, 0.75 - (frac - 0.5) ** 2, 0.5 * frac * frac])
    slopes = jnp.stack([frac - 1.0, 1.0 - 2.0 * frac, frac])
    return weights, slopes


def rounded(value):
    return value.astype(jnp.bfloat16).astype(jnp.float32)


def reference(brick_ids, voxel_offset, fractions, normals, point_weight, tile_count):
    pad_y = NY + 2
    pad_z = NZ + 2
    total = (NX + 2) * pad_y * pad_z
    dest_all = brick_ids[:, 0].reshape(DEVICES, TILES_DEV)
    off_all = voxel_offset.reshape(DEVICES, TILES_DEV, TILE)
    frac_all = fractions.reshape(DEVICES, TILES_DEV, 3, TILE)
    norm_all = normals.reshape(DEVICES, TILES_DEV, 3, TILE)
    weight_all = point_weight.reshape(DEVICES, TILES_DEV, TILE)
    stencil = jnp.arange(3, dtype=jnp.int32)

    def step(carry, items):
        rhs_flat, screen_flat = carry
        dest, offset, frac, normal, weight, count = items
        valid = (jnp.arange(TILES_DEV, dtype=jnp.int32) < count).astype(jnp.float32)[:, None]
        normal = normal * valid[:, None, :]
        weight = weight * valid
        cell_x = offset // (BY * BZ)
        cell_y = (offset // BZ) % BY
        cell_z = offset % BZ
        base_x = (dest // N_YZ)[:, None] * BX + cell_x
        base_y = (dest % N_YZ)[:, None] * BY + cell_y
        wx, gx = spline(frac[:, 0])
        wy, gy = spline(frac[:, 1])
        wz, gz = spline(frac[:, 2])
        nx = normal[:, 0]
        ny = normal[:, 1]
        nz = normal[:, 2]
        a12 = rounded(nx[None, None] * gx[:, None] * wy[None, :] + ny[None, None] * wx[:, None] * gy[None, :])
        a3 = rounded(nz[None, None] * wx[:, None] * wy[None, :])
        a_s = rounded(weight[None, None] * wx[:, None] * wy[None, :])
        zb = rounded(wz)
        zd = rounded(gz)
        rhs_terms = a12[:, :, None] * zb[None, None] + a3[:, :, None] * zd[None, None]
        screen_terms = a_s[:, :, None] * zb[None, None]
        index = ((base_x[None, None, None] + stencil[:, None, None, None, None]) * pad_y
                 + base_y[None, None, None] + stencil[None, :, None, None, None]) * pad_z \
            + cell_z[None, None, None] + stencil[None, None, :, None, None]
        index = index.astype(jnp.int32).ravel()
        rhs_flat = rhs_flat.at[index].add(rhs_terms.ravel())
        screen_flat = screen_flat.at[index].add(screen_terms.ravel())
        return (rhs_flat, screen_flat), None

    start = (jnp.zeros((total,), jnp.float32), jnp.zeros((total,), jnp.float32))
    (rhs_flat, screen_flat), _ = lax.scan(step, start, (dest_all, off_all, frac_all, norm_all, weight_all, tile_count))
    rhs = rhs_flat.reshape(NX + 2, pad_y, pad_z)[1:-1, 1:-1, 1:-1]
    screen = screen_flat.reshape(NX + 2, pad_y, pad_z)[1:-1, 1:-1, 1:-1]
    return (rhs, screen)
```

```python
import jax
import jax.numpy as jnp
from jax import lax
from jax.experimental import pallas as pl
from jax.experimental.pallas import tpu as pltpu
from jax.sharding import PartitionSpec as P

BX = 4
BY = 8
BZ = 128
CAP = 2
ROWS = 8 * (BY + 2)
GROUP = 4


def passed_along(value, axis, steps):
    count = lax.axis_size(axis)
    first, last = (max(0, -steps), min(count, count - steps))
    return lax.ppermute(value, axis, [(source, source + steps) for source in range(first, last)])


def dispatch_kernel(ids_ref, count_ref, offset_ref, frac_ref, normal_ref, weight_ref, out_ref, seen_ref):
    slots = out_ref.shape[0]

    def clear(i, _):
        out_ref[pl.ds(i * 8, 8)] = jnp.zeros((8,) + out_ref.shape[1:], jnp.float32)
        return 0

    lax.fori_loop(0, slots // 8, clear, 0)

    def reset(i, _):
        seen_ref[i] = 0
        return 0

    lax.fori_loop(0, seen_ref.shape[0], reset, 0)

    def place(t, _):
        brick = ids_ref[t]
        rank = seen_ref[brick]
        seen_ref[brick] = rank + 1
        slot = brick * CAP + jnp.minimum(rank, CAP - 1)
        out_ref[slot, 0:3, :] = frac_ref[t]
        out_ref[slot, 3:4, :] = offset_ref[pl.ds(t, 1), :].astype(jnp.float32)
        out_ref[slot, 4:7, :] = normal_ref[t]
        out_ref[slot, 7:8, :] = weight_ref[pl.ds(t, 1), :]
        return 0

    lax.fori_loop(0, jnp.minimum(count_ref[0], ids_ref.shape[0]), place, 0)


def dispatch(ids, count, offset, frac, normal, weight, bricks):
    smem = pl.BlockSpec(memory_space=pltpu.SMEM)
    vmem = pl.BlockSpec(memory_space=pltpu.VMEM)
    return pl.pallas_call(
        dispatch_kernel,
        out_shape=jax.ShapeDtypeStruct((bricks * CAP, 8, offset.shape[1]), jnp.float32),
        in_specs=[smem, smem, vmem, vmem, vmem, vmem],
        out_specs=vmem,
        scratch_shapes=[pltpu.SMEM((bricks,), jnp.int32)],
        name="dispatch",
    )(ids, count, offset, frac, normal, weight)


def bspline(t):
    outer = jnp.maximum(1.5 - jnp.abs(t), 0.0)
    inner = jnp.maximum(outer - 1.0, 0.0)
    value = outer * outer - 3.0 * (inner * inner)
    slope = jnp.minimum(jnp.maximum(t + t, -outer), outer)
    return value, slope


def build(inbox_ref, tile, lanes, y_ref, a_ref, z_ref, col):
    def row(c):
        return jnp.broadcast_to(inbox_ref[tile, c : c + 1, lanes], (8, 128))

    sub = lax.broadcasted_iota(jnp.int32, (8, 128), 0).astype(jnp.float32)
    offset = row(3).astype(jnp.int32)
    cell_x = lax.shift_right_logical(offset, 10).astype(jnp.float32)
    cell_y = (lax.shift_right_logical(offset, 7) & 7).astype(jnp.float32)
    cell_z = (offset & 127).astype(jnp.float32)
    x_value, x_slope = bspline((sub - 0.5) - (cell_x + row(0)))
    at_y = cell_y + row(1)
    for half in range(2):
        y_value, y_slope = bspline((sub + (8 * half - 0.5)) - at_y)
        y_ref[8 * half : 8 * half + 8, :] = y_value
        y_ref[16 + 8 * half : 24 + 8 * half, :] = y_slope
    one = row(4) * x_slope
    two = row(5) * x_value
    three = row(6) * x_value
    screen = row(7) * x_value
    cols = pl.ds(col, 128)
    for pair in range((BY + 2) // 2):
        planes = [[], [], []]
        for s in (2 * pair, 2 * pair + 1):
            yv = jnp.broadcast_to(y_ref[s : s + 1, :], (8, 128))
            ys = jnp.broadcast_to(y_ref[16 + s : 17 + s, :], (8, 128))
            planes[0].append(one * yv + two * ys)
            planes[1].append(three * yv)
            planes[2].append(screen * yv)
        for k in range(3):
            a_ref[k * ROWS + 16 * pair : k * ROWS + 16 * pair + 16, cols] = jnp.concatenate(
                planes[k], axis=0
            ).astype(jnp.bfloat16)
    fz = row(2)

    def half_row(v):
        return jnp.concatenate([v, v], axis=0).astype(jnp.bfloat16)

    weights = [half_row(0.5 * (1.0 - fz) * (1.0 - fz)), half_row(0.75 - (fz - 0.5) * (fz - 0.5)), half_row(0.5 * fz * fz)]
    slopes = [half_row(fz - 1.0), half_row(1.0 - 2.0 * fz), half_row(fz)]
    where = [half_row(cell_z - 1.0), half_row(cell_z), half_row(cell_z + 1.0)]
    zero = jnp.zeros((16, 128), jnp.bfloat16)
    depth = lax.broadcasted_iota(jnp.int32, (16, 128), 0).astype(jnp.float32)
    for block in range(BZ // 16):
        here = (depth + 16.0 * block).astype(jnp.bfloat16)
        hits = [here == w for w in where]
        value = jnp.where(hits[0], weights[0], jnp.where(hits[1], weights[1], jnp.where(hits[2], weights[2], zero)))
        slope = jnp.where(hits[0], slopes[0], jnp.where(hits[1], slopes[1], jnp.where(hits[2], slopes[2], zero)))
        z_ref[16 * block : 16 * block + 16, cols] = value
        z_ref[BZ + 16 * block : BZ + 16 * block + 16, cols] = slope


def splat_kernel(inbox_ref, out_ref, acc_ref, y_ref, a0, z0, a1, z1):
    slots, _, points = inbox_ref.shape
    steps = slots // GROUP

    def fill(step, a_ref, z_ref):
        for g in range(GROUP):
            for h in range(points // 128):
                build(inbox_ref, step * GROUP + g, pl.ds(128 * h, 128), y_ref, a_ref, z_ref, g * points + 128 * h)

    def product(a_ref, z_ref):
        acc_ref[...] += lax.dot_general(
            a_ref[...], z_ref[...], (((1,), (1,)), ((), ())), preferred_element_type=jnp.float32
        )

    acc_ref[...] = jnp.zeros_like(acc_ref)
    fill(0, a0, z0)

    def body(i, _):
        product(a0, z0)
        fill(2 * i + 1, a1, z1)
        product(a1, z1)
        fill(jnp.minimum(2 * i + 2, steps - 1), a0, z0)
        return 0

    lax.fori_loop(0, steps // 2, body, 0)
    out_ref[0] = 0.5 * acc_ref[0:ROWS, 0:BZ] + 0.25 * acc_ref[ROWS : 2 * ROWS, BZ : 2 * BZ]
    out_ref[1] = 0.25 * acc_ref[2 * ROWS : 3 * ROWS, 0:BZ]


def splat(inbox):
    points = inbox.shape[2]
    width = GROUP * points
    vmem = pl.BlockSpec(memory_space=pltpu.VMEM)
    return pl.pallas_call(
        splat_kernel,
        out_shape=jax.ShapeDtypeStruct((2, ROWS, BZ), jnp.float32),
        in_specs=[vmem],
        out_specs=vmem,
        scratch_shapes=[
            pltpu.VMEM((3 * ROWS, 2 * BZ), jnp.float32),
            pltpu.VMEM((32, 128), jnp.float32),
            pltpu.VMEM((3 * ROWS, width), jnp.bfloat16),
            pltpu.VMEM((2 * BZ, width), jnp.bfloat16),
            pltpu.VMEM((3 * ROWS, width), jnp.bfloat16),
            pltpu.VMEM((2 * BZ, width), jnp.bfloat16),
        ],
        name="splat",
    )(inbox)


def shards(brick_ids, voxel_offset, fractions, normals, point_weight, tile_count):
    bricks = lax.axis_size("gx") * lax.axis_size("yz")
    outbox = dispatch(brick_ids[:, 0], tile_count, voxel_offset, fractions, normals, point_weight, bricks)
    inbox = lax.all_to_all(outbox, ("gx", "yz"), split_axis=0, concat_axis=0, tiled=True)
    field = splat(inbox).reshape(2, BY + 2, 8, BZ)
    from_below = passed_along(field[:, :, BX + 1], "gx", 1)
    from_above = passed_along(field[:, :, 0], "gx", -1)
    rows = [field[:, :, r] for r in range(1, BX + 1)]
    rows[0] = rows[0] + from_below
    rows[-1] = rows[-1] + from_above
    inner = jnp.stack(rows, axis=1)
    from_left = passed_along(inner[:, :, BY + 1], "yz", 1)
    from_right = passed_along(inner[:, :, 0], "yz", -1)
    middle = inner[:, :, 1 : BY + 1]
    left = jnp.pad(from_left[:, :, None], ((0, 0), (0, 0), (0, BY - 1), (0, 0)))
    right = jnp.pad(from_right[:, :, None], ((0, 0), (0, 0), (BY - 1, 0), (0, 0)))
    result = middle + left + right
    return (result[0], result[1])


def solution(mesh):
    return jax.shard_map(
        shards,
        mesh=mesh,
        in_specs=(
            P(("gx", "yz"), None),
            P(("gx", "yz"), None),
            P(("gx", "yz"), None, None),
            P(("gx", "yz"), None, None),
            P(("gx", "yz"), None),
            P(("gx", "yz")),
        ),
        out_specs=(P("gx", "yz", None), P("gx", "yz", None)),
        check_vma=False,
    )
```

```python
import jax
import jax.numpy as jnp
from jax import lax
from jax.experimental import pallas as pl
from jax.experimental.pallas import tpu as pltpu
from jax.sharding import PartitionSpec as P

BX = 4
BY = 8
BZ = 128
CAP = 2
ROWS = 64
GROUP = 8
LANES = 128


def passed_along(value, axis, steps):
    count = lax.axis_size(axis)
    first, last = (max(0, -steps), min(count, count - steps))
    return lax.ppermute(value, axis, [(source, source + steps) for source in range(first, last)])


def dispatch_kernel(ids_ref, count_ref, offset_ref, frac_ref, normal_ref, weight_ref, out_ref, seen_ref):
    slots = out_ref.shape[0]

    def clear(i, _):
        out_ref[pl.ds(i * 8, 8)] = jnp.zeros((8,) + out_ref.shape[1:], jnp.float32)
        return 0

    lax.fori_loop(0, slots // 8, clear, 0)

    def reset(i, _):
        seen_ref[i] = 0
        return 0

    lax.fori_loop(0, seen_ref.shape[0], reset, 0)

    def place(t, _):
        brick = ids_ref[t]
        rank = seen_ref[brick]
        seen_ref[brick] = rank + 1
        slot = brick * CAP + jnp.minimum(rank, CAP - 1)
        here = pl.ds(t, 1)
        rows = [frac_ref[k, here, :] for k in range(3)] + [offset_ref[here, :].astype(jnp.float32)]
        rows += [normal_ref[k, here, :] for k in range(3)] + [weight_ref[here, :]]
        for half in range(out_ref.shape[1] // 8):
            for k, row in enumerate(rows):
                out_ref[slot, 8 * half + k : 8 * half + k + 1, :] = row[:, LANES * half : LANES * half + LANES]
        return 0

    lax.fori_loop(0, jnp.minimum(count_ref[0], ids_ref.shape[0]), place, 0)


def dispatch(ids, count, offset, frac, normal, weight, bricks):
    smem = pl.BlockSpec(memory_space=pltpu.SMEM)
    vmem = pl.BlockSpec(memory_space=pltpu.VMEM)
    return pl.pallas_call(
        dispatch_kernel,
        out_shape=jax.ShapeDtypeStruct((bricks * CAP, 8 * offset.shape[1] // LANES, LANES), jnp.float32),
        in_specs=[smem, smem, vmem, vmem, vmem, vmem],
        out_specs=vmem,
        scratch_shapes=[pltpu.SMEM((bricks,), jnp.int32)],
        name="dispatch",
    )(ids, count, offset, frac, normal, weight)


def bspline(t):
    outer = jnp.maximum(1.5 - jnp.abs(t), 0.0)
    inner = jnp.maximum(outer - 1.0, 0.0)
    value = outer * outer - 3.0 * (inner * inner)
    slope = jnp.minimum(jnp.maximum(t + t, -outer), outer)
    return value, slope


def prepare(inbox_ref, group, half, prep_ref):
    per_tile = 8 * prep_ref.shape[0]

    def channel(c):
        return inbox_ref[pl.ds(group * (per_tile * GROUP) + 8 * half + c, GROUP, stride=per_tile), :]

    offset = channel(3).astype(jnp.int32)
    at_x = lax.shift_right_logical(offset, 10).astype(jnp.float32) + channel(0)
    at_y = (lax.shift_right_logical(offset, 7) & 7).astype(jnp.float32) + channel(1)
    rows = [at_x, at_y]
    for s in (BY, BY + 1):
        rows.extend(bspline((s - 0.5) - at_y))
    fz = channel(2)
    rows.extend([0.5 * (1.0 - fz) * (1.0 - fz), 0.75 - (fz - 0.5) * (fz - 0.5), 0.5 * fz * fz])
    rows.extend([fz - 1.0, 1.0 - 2.0 * fz, fz])
    cell_z = offset & 127
    for k in (-1, 0, 1):
        rows.append(((cell_z + k) & 15).astype(jnp.float32))
    for k in (-1, 0, 1):
        rows.append(lax.shift_right_arithmetic(cell_z + k, 4).astype(jnp.float32))
    rows.extend([channel(4), channel(5), channel(6), channel(7)])
    for i, row in enumerate(rows):
        prep_ref[half, i] = row


def build(prep_ref, half, tile, x_ref):
    def row(i):
        return jnp.broadcast_to(prep_ref[half, i, tile : tile + 1, :], (8, LANES))

    def paired(i):
        v = row(i)
        return jnp.concatenate([v, v], axis=0).astype(jnp.bfloat16)

    sub = lax.broadcasted_iota(jnp.int32, (8, LANES), 0).astype(jnp.float32) - 0.5
    x_value, x_slope = bspline(sub - row(0))
    y_value, y_slope = bspline(sub - row(1))
    factors = [row(18) * x_slope, row(19) * x_value, row(20) * x_value, row(21) * x_value]
    for i, v in enumerate(factors):
        x_ref[i] = v

    def planes(one, two, three, screen, yv, ys):
        return [one * yv + two * ys, three * yv, screen * yv]

    left = [[], [], []]
    for pair in range(4):
        blocks = []
        for p in (2 * pair, 2 * pair + 1):
            if p < BX + 2:
                wide = [jnp.broadcast_to(x_ref[i, p : p + 1, :], (8, LANES)) for i in range(4)]
                blocks.append(planes(*wide, y_value, y_slope))
            else:
                s = p - (BX + 2)
                blocks.append(planes(*factors, row(2 + 2 * s), row(3 + 2 * s)))
        for k in range(3):
            left[k].append(jnp.concatenate([blocks[0][k], blocks[1][k]], axis=0).astype(jnp.bfloat16))

    zero = jnp.zeros((16, LANES), jnp.bfloat16)
    depth = lax.broadcasted_iota(jnp.int32, (16, LANES), 0).astype(jnp.float32).astype(jnp.bfloat16)
    hits = [depth == paired(12 + k) for k in range(3)]

    def pick(first, default):
        return jnp.where(hits[0], paired(first), jnp.where(hits[1], paired(first + 1), default))

    value = pick(6, jnp.where(hits[2], paired(8), zero))
    slope = pick(9, jnp.where(hits[2], paired(11), zero))
    home = pick(15, paired(17))
    right = [[], []]
    for block in range(BZ // 16):
        inside = home == jnp.full((16, LANES), block, jnp.bfloat16)
        right[0].append(jnp.where(inside, value, zero))
        right[1].append(jnp.where(inside, slope, zero))
    return jnp.concatenate(sum(left, []), axis=0), jnp.concatenate(sum(right, []), axis=0)


def splat_kernel(inbox_ref, field_ref, up_ref, down_ref, acc_ref, prep_ref, x_ref):
    halves = prep_ref.shape[0]
    slots = inbox_ref.shape[0] // (8 * halves)
    acc_ref[...] = jnp.zeros_like(acc_ref)

    def body(group, _):
        for half in range(halves):
            prepare(inbox_ref, group, half, prep_ref)
        acc = acc_ref[...]
        for tile in range(GROUP):
            sides = [build(prep_ref, half, tile, x_ref.at[(tile * halves + half) % 4]) for half in range(halves)]
            acc = acc + lax.dot_general(
                jnp.concatenate([a for a, _ in sides], axis=1),
                jnp.concatenate([z for _, z in sides], axis=1),
                (((1,), (1,)), ((), ())),
                preferred_element_type=jnp.float32,
            )
        acc_ref[...] = acc
        return 0

    lax.fori_loop(0, slots // GROUP, body, 0)
    field_ref[0] = 0.5 * acc_ref[0:ROWS, 0:BZ] + 0.25 * acc_ref[ROWS : 2 * ROWS, BZ : 2 * BZ]
    field_ref[1] = 0.25 * acc_ref[2 * ROWS : 3 * ROWS, 0:BZ]
    tail = jnp.zeros((4, BZ), jnp.float32)
    for ref, r in ((up_ref, BX + 1), (down_ref, 0)):
        for c in range(2):
            ref[8 * c : 8 * c + 8, :] = field_ref[c, 8 * r : 8 * r + 8, :]
            for s in range(2):
                ref[16 + 2 * c + s : 17 + 2 * c + s, :] = field_ref[c, 48 + 8 * s + r : 49 + 8 * s + r, :]
        ref[20:24, :] = tail


def splat(inbox, halves):
    vmem = pl.BlockSpec(memory_space=pltpu.VMEM)
    return pl.pallas_call(
        splat_kernel,
        out_shape=(
            jax.ShapeDtypeStruct((2, ROWS, BZ), jnp.float32),
            jax.ShapeDtypeStruct((24, BZ), jnp.float32),
            jax.ShapeDtypeStruct((24, BZ), jnp.float32),
        ),
        in_specs=[vmem],
        out_specs=(vmem, vmem, vmem),
        scratch_shapes=[
            pltpu.VMEM((3 * ROWS, 2 * BZ), jnp.float32),
            pltpu.VMEM((halves, 22, GROUP, LANES), jnp.float32),
            pltpu.VMEM((4, 4, 8, LANES), jnp.float32),
        ],
        name="splat",
    )(inbox)


def face_rows(face):
    ends = face[16:20].reshape(2, 2, BZ)
    return jnp.concatenate([face[0:16].reshape(2, BY, BZ), ends], axis=1)


def shards(brick_ids, voxel_offset, fractions, normals, point_weight, tile_count):
    bricks = lax.axis_size("gx") * lax.axis_size("yz")
    outbox = dispatch(
        brick_ids[:, 0],
        tile_count,
        voxel_offset,
        jnp.transpose(fractions, (1, 0, 2)),
        jnp.transpose(normals, (1, 0, 2)),
        point_weight,
        bricks,
    )
    inbox = lax.all_to_all(outbox, ("gx", "yz"), split_axis=0, concat_axis=0, tiled=True)
    field, up, down = splat(inbox.reshape(-1, LANES), inbox.shape[1] // 8)
    from_below = passed_along(up, "gx", 1)
    from_above = passed_along(down, "gx", -1)
    main = field[:, 8 : 8 * (BX + 1)].reshape(2, BX, BY, BZ)
    ends = field[:, 48:64].reshape(2, 2, 8, BZ)[:, :, 1 : BX + 1]
    inner = jnp.concatenate([main, jnp.transpose(ends, (0, 2, 1, 3))], axis=2)
    inner = jnp.concatenate(
        [
            inner[:, :1] + face_rows(from_below)[:, None],
            inner[:, 1 : BX - 1],
            inner[:, BX - 1 :] + face_rows(from_above)[:, None],
        ],
        axis=1,
    )
    from_left = passed_along(inner[:, :, BY + 1].reshape(2 * BX, BZ), "yz", 1).reshape(2, BX, 1, BZ)
    from_right = passed_along(inner[:, :, 0].reshape(2 * BX, BZ), "yz", -1).reshape(2, BX, 1, BZ)
    result = jnp.concatenate(
        [inner[:, :, 1:2] + from_left, inner[:, :, 2:BY], inner[:, :, BY : BY + 1] + from_right], axis=2
    )
    return (result[0], result[1])


def solution(mesh):
    return jax.shard_map(
        shards,
        mesh=mesh,
        in_specs=(
            P(("gx", "yz"), None),
            P(("gx", "yz"), None),
            P(("gx", "yz"), None, None),
            P(("gx", "yz"), None, None),
            P(("gx", "yz"), None),
            P(("gx", "yz")),
        ),
        out_specs=(P("gx", "yz", None), P("gx", "yz", None)),
        check_vma=False,
    )
```

```python
import jax
import jax.numpy as jnp
from jax import lax
from jax.experimental import pallas as pl
from jax.experimental.pallas import tpu as pltpu
from jax.sharding import PartitionSpec as P

BX = 4
BY = 8
BZ = 128
CAP = 2
LANES = 128
GROUP = 8
UNROLL = 8
PLANES = (BX + 2) * BY
ENDS = 16
ROWS = PLANES + ENDS
ROW_X = 0
ROW_Z = 4 * (BX + 2)
ROW_COUNT = ROW_Z + 8
SIDES = 8


def passed_along(value, axis, steps):
    count = lax.axis_size(axis)
    return lax.ppermute(value, axis, [(source, (source + steps) % count) for source in range(count)])


def dispatch_kernel(ids_ref, count_ref, offset_ref, frac_ref, normal_ref, weight_ref, out_ref, seen_ref):
    slots = out_ref.shape[0]

    def clear(i, _):
        out_ref[pl.ds(i * 8, 8)] = jnp.zeros((8,) + out_ref.shape[1:], jnp.float32)
        return 0

    lax.fori_loop(0, slots // 8, clear, 0)

    def reset(i, _):
        seen_ref[i] = 0
        return 0

    lax.fori_loop(0, seen_ref.shape[0], reset, 0)

    def place(t, _):
        brick = ids_ref[t]
        rank = seen_ref[brick]
        seen_ref[brick] = rank + 1
        slot = brick * CAP + jnp.minimum(rank, CAP - 1)
        here = pl.ds(t, 1)
        rows = [frac_ref[k, here, :] for k in range(3)] + [offset_ref[here, :].astype(jnp.float32)]
        rows += [normal_ref[k, here, :] for k in range(3)] + [weight_ref[here, :]]
        for half in range(out_ref.shape[1] // 8):
            for k, row in enumerate(rows):
                out_ref[slot, 8 * half + k : 8 * half + k + 1, :] = row[:, LANES * half : LANES * half + LANES]
        return 0

    lax.fori_loop(0, jnp.minimum(count_ref[0], ids_ref.shape[0]), place, 0)


def dispatch(ids, count, offset, frac, normal, weight, bricks):
    smem = pl.BlockSpec(memory_space=pltpu.SMEM)
    vmem = pl.BlockSpec(memory_space=pltpu.VMEM)
    return pl.pallas_call(
        dispatch_kernel,
        out_shape=jax.ShapeDtypeStruct((bricks * CAP, 8 * offset.shape[1] // LANES, LANES), jnp.float32),
        in_specs=[smem, smem, vmem, vmem, vmem, vmem],
        out_specs=vmem,
        scratch_shapes=[pltpu.SMEM((bricks,), jnp.int32)],
        name="dispatch",
    )(ids, count, offset, frac, normal, weight)


def spline(f):
    return (
        [0.5 * (1.0 - f) * (1.0 - f), 0.75 - (f - 0.5) * (f - 0.5), 0.5 * f * f],
        [f - 1.0, 1.0 - 2.0 * f, f],
    )


def spread(cell, cells, pieces):
    here = [cell == c for c in range(cells)]
    out = []
    for target in range(cells + 2):
        value = None
        for i in range(3):
            c = target - i
            if 0 <= c < cells:
                value = jnp.where(here[c], pieces[i], 0.0 if value is None else value)
        out.append(value)
    return out


def prepare(inbox_ref, first, row_ref, side_ref):
    def channel(c):
        return inbox_ref[pl.ds(first * 8 + c, GROUP, stride=8), :]

    offset = channel(3).astype(jnp.int32)
    weights, slopes = spline(channel(0))
    cell = lax.shift_right_logical(offset, 10)
    x_value, x_slope = spread(cell, BX, weights), spread(cell, BX, slopes)
    weights, slopes = spline(channel(1))
    cell = lax.shift_right_logical(offset, 7) & 7
    y_value, y_slope = spread(cell, BY, weights), spread(cell, BY, slopes)
    nx, ny, nz, weight = [channel(c) for c in (4, 5, 6, 7)]
    for r in range(BX + 2):
        parts = (nx * x_slope[r], ny * x_value[r], nz * x_value[r], weight * x_value[r])
        for i, part in enumerate(parts):
            row_ref[ROW_X + 4 * r + i] = part
        for e in range(2):
            yv, ys = y_value[BY + e], y_slope[BY + e]
            ends = (parts[0] * yv + parts[1] * ys, parts[2] * yv, parts[3] * yv)
            for k in range(3):
                side_ref[2 * k + e, GROUP * r : GROUP * r + GROUP, :] = ends[k]
    for s in range(BY):
        side_ref[6, GROUP * s : GROUP * s + GROUP, :] = y_value[s]
        side_ref[7, GROUP * s : GROUP * s + GROUP, :] = y_slope[s]
    weights, slopes = spline(channel(2))
    cell = offset & 127
    rows = weights + slopes + [(cell & 15).astype(jnp.float32), lax.shift_right_logical(cell, 4).astype(jnp.float32)]
    for i, row in enumerate(rows):
        row_ref[ROW_Z + i] = row


def build(row_ref, side_ref, unit):
    def row(i):
        return jnp.broadcast_to(row_ref[i, unit : unit + 1, :], (8, LANES))

    def paired(i):
        v = row(i)
        return jnp.concatenate([v, v], axis=0).astype(jnp.bfloat16)

    def side(i):
        return side_ref[i, pl.ds(unit, 8, stride=GROUP), :]

    y_value, y_slope = side(6), side(7)
    left = [[], [], []]
    for pair in range((BX + 2) // 2):
        blocks = []
        for r in (2 * pair, 2 * pair + 1):
            one, two, three, screen = [row(ROW_X + 4 * r + i) for i in range(4)]
            blocks.append((one * y_value + two * y_slope, three * y_value, screen * y_value))
        for k in range(3):
            left[k].append(jnp.concatenate([blocks[0][k], blocks[1][k]], axis=0).astype(jnp.bfloat16))
    for k in range(3):
        left[k].append(jnp.concatenate([side(2 * k), side(2 * k + 1)], axis=0).astype(jnp.bfloat16))

    depth = lax.broadcasted_iota(jnp.int32, (16, LANES), 0)
    zero = jnp.zeros((16, LANES), jnp.bfloat16)

    def constant(v):
        return v.astype(jnp.float32).astype(jnp.bfloat16)

    low, block_of = paired(ROW_Z + 6), paired(ROW_Z + 7)
    w = [paired(ROW_Z + i) for i in range(6)]
    below = constant((depth + 1) & 15) == low
    value, slope = jnp.where(below, w[0], zero), jnp.where(below, w[3], zero)
    carry = jnp.where(below, constant(jnp.where(depth == 15, -1, 0)), zero)
    same = constant(depth) == low
    value, slope = jnp.where(same, w[1], value), jnp.where(same, w[4], slope)
    above = constant((depth + 15) & 15) == low
    value, slope = jnp.where(above, w[2], value), jnp.where(above, w[5], slope)
    home = block_of + jnp.where(above, constant(jnp.where(depth == 0, 1, 0)), carry)
    right = [[], []]
    for block in range(BZ // 16):
        inside = home == jnp.full((16, LANES), block, jnp.bfloat16)
        right[0].append(jnp.where(inside, value, zero))
        right[1].append(jnp.where(inside, slope, zero))
    return jnp.concatenate(sum(left, []), axis=0), jnp.concatenate(sum(right, []), axis=0)


def splat_kernel(inbox_ref, field_ref, up_ref, down_ref, right_ref, left_ref, acc_ref, row_ref, side_ref):
    batch = GROUP * UNROLL
    steps = inbox_ref.shape[0] // (8 * batch)

    acc_ref[...] = jnp.zeros_like(acc_ref)

    def body(i, _):
        for u in range(UNROLL):
            prepare(inbox_ref, i * batch + u * GROUP, row_ref.at[u], side_ref.at[u])
        acc = acc_ref[...]
        for pair in range(batch // 2):
            sides = [build(row_ref.at[k // GROUP], side_ref.at[k // GROUP], k % GROUP) for k in (2 * pair, 2 * pair + 1)]
            acc = acc + lax.dot_general(
                jnp.concatenate([a for a, _ in sides], axis=1),
                jnp.concatenate([z for _, z in sides], axis=1),
                (((1,), (1,)), ((), ())),
                preferred_element_type=jnp.float32,
            )
        acc_ref[...] = acc
        return 0

    lax.fori_loop(0, steps, body, 0)
    for k in range(2):
        first = 2 * ROWS * k
        if k == 0:
            acc_ref[0:ROWS, 0:BZ] = acc_ref[0:ROWS, 0:BZ] + acc_ref[ROWS : 2 * ROWS, BZ : 2 * BZ]

        def rows(at, count, first=first):
            return acc_ref[first + at : first + at + count, 0:BZ]

        for r in range(BX):
            field_ref[k, r, 0 : BY - 1, :] = rows(BY * (r + 1) + 1, BY - 1)
            field_ref[k, r, BY - 1 : BY, :] = rows(PLANES + r + 1, 1)
            left_ref[BX * k + r : BX * k + r + 1, :] = rows(BY * (r + 1), 1)
        right_ref[BX * k : BX * k + BX, :] = rows(PLANES + 9, BX)
        for ref, r in ((up_ref, BX + 1), (down_ref, 0)):
            ref[BY * k : BY * k + BY - 1, :] = rows(BY * r + 1, BY - 1)
            ref[BY * k + BY - 1 : BY * k + BY, :] = rows(PLANES + r, 1)
            ref[16 + k : 17 + k, :] = rows(BY * r, 1)
            ref[18 + k : 19 + k, :] = rows(PLANES + 8 + r, 1)
    for ref in (up_ref, down_ref):
        ref[20:24, :] = jnp.zeros((4, BZ), jnp.float32)


def splat(inbox):
    vmem = pl.BlockSpec(memory_space=pltpu.VMEM)
    shapes = ((2, BX, BY, BZ), (24, BZ), (24, BZ), (2 * BX, BZ), (2 * BX, BZ))
    return pl.pallas_call(
        splat_kernel,
        out_shape=tuple(jax.ShapeDtypeStruct(shape, jnp.float32) for shape in shapes),
        in_specs=[vmem],
        out_specs=(vmem,) * len(shapes),
        scratch_shapes=[
            pltpu.VMEM((3 * ROWS, 2 * BZ), jnp.float32),
            pltpu.VMEM((UNROLL, ROW_COUNT, GROUP, LANES), jnp.float32),
            pltpu.VMEM((UNROLL, SIDES, 8 * GROUP, LANES), jnp.float32),
        ],
        compiler_params=pltpu.CompilerParams(vmem_limit_bytes=16 * 1024 * 1024),
        name="splat",
    )(inbox)


def join_kernel(edge_ref, below_ref, above_ref, right_ref, left_ref, right_out, left_out):
    below = jnp.where(edge_ref[0] == 0, 0.0, below_ref[16:24, :])
    above = jnp.where(edge_ref[1] == 0, 0.0, above_ref[16:24, :])
    right_out[...] = right_ref[...]
    left_out[...] = left_ref[...]
    for k in range(2):
        for out, at in ((left_out, k), (right_out, 2 + k)):
            first, last = BX * k, BX * k + BX - 1
            out[first : first + 1, :] = out[first : first + 1, :] + below[at : at + 1]
            out[last : last + 1, :] = out[last : last + 1, :] + above[at : at + 1]


def join(edges, below, above, right, left):
    smem = pl.BlockSpec(memory_space=pltpu.SMEM)
    vmem = pl.BlockSpec(memory_space=pltpu.VMEM)
    shape = jax.ShapeDtypeStruct(right.shape, jnp.float32)
    return pl.pallas_call(
        join_kernel,
        out_shape=(shape, shape),
        in_specs=[smem] + [vmem] * 4,
        out_specs=(vmem, vmem),
        compiler_params=pltpu.CompilerParams(vmem_limit_bytes=4 * 1024 * 1024),
        name="join",
    )(edges, below, above, right, left)


def finish_kernel(edge_ref, field_ref, below_ref, above_ref, before_ref, after_ref, rhs_ref, screen_ref):
    for k, ref in enumerate((rhs_ref, screen_ref)):
        for r in range(BX):
            plane = field_ref[k, r]
            if r == 0:
                plane = plane + jnp.where(edge_ref[0] == 0, 0.0, below_ref[BY * k : BY * k + BY, :])
            if r == BX - 1:
                plane = plane + jnp.where(edge_ref[1] == 0, 0.0, above_ref[BY * k : BY * k + BY, :])
            ref[r] = plane
            at = BX * k + r
            before = jnp.where(edge_ref[2] == 0, 0.0, before_ref[at : at + 1, :])
            after = jnp.where(edge_ref[3] == 0, 0.0, after_ref[at : at + 1, :])
            ref[r, 0:1, :] = ref[r, 0:1, :] + before
            ref[r, BY - 1 : BY, :] = ref[r, BY - 1 : BY, :] + after


def finish(edges, field, below, above, before, after):
    smem = pl.BlockSpec(memory_space=pltpu.SMEM)
    vmem = pl.BlockSpec(memory_space=pltpu.VMEM)
    shape = jax.ShapeDtypeStruct((BX, BY, BZ), jnp.float32)
    return pl.pallas_call(
        finish_kernel,
        out_shape=(shape, shape),
        in_specs=[smem] + [vmem] * 5,
        out_specs=(vmem, vmem),
        compiler_params=pltpu.CompilerParams(vmem_limit_bytes=4 * 1024 * 1024),
        name="finish",
    )(edges, field, below, above, before, after)


def shards(brick_ids, voxel_offset, fractions, normals, point_weight, tile_count):
    slabs, columns = lax.axis_size("gx"), lax.axis_size("yz")
    outbox = dispatch(
        brick_ids[:, 0],
        tile_count,
        voxel_offset,
        jnp.transpose(fractions, (1, 0, 2)),
        jnp.transpose(normals, (1, 0, 2)),
        point_weight,
        slabs * columns,
    )
    inbox = lax.all_to_all(outbox, ("gx", "yz"), split_axis=0, concat_axis=0, tiled=True)
    slab, column = lax.axis_index("gx"), lax.axis_index("yz")
    edges = jnp.stack([slab, slabs - 1 - slab, column, columns - 1 - column])
    field, up, down, right, left = splat(inbox.reshape(-1, LANES))
    below = passed_along(up, "gx", 1)
    above = passed_along(down, "gx", -1)
    right, left = join(edges, below, above, right, left)
    before = passed_along(right, "yz", 1)
    after = passed_along(left, "yz", -1)
    return finish(edges, field, below, above, before, after)


def solution(mesh):
    return jax.shard_map(
        shards,
        mesh=mesh,
        in_specs=(
            P(("gx", "yz"), None),
            P(("gx", "yz"), None),
            P(("gx", "yz"), None, None),
            P(("gx", "yz"), None, None),
            P(("gx", "yz"), None),
            P(("gx", "yz")),
        ),
        out_specs=(P("gx", "yz", None), P("gx", "yz", None)),
        check_vma=False,
    )
```

```python
import jax
import jax.numpy as jnp
from jax import lax
from jax.experimental import pallas as pl
from jax.experimental.pallas import tpu as pltpu
from jax.sharding import PartitionSpec as P

BX = 4
BY = 8
BZ = 128
CAP = 2
LANES = 128
GROUP = 8
UNROLL = 16
PLANES = (BX + 2) * BY
ENDS = 16
ROWS = PLANES + ENDS
ROW_X = 0
ROW_Z = 4 * (BX + 2)
ROW_COUNT = ROW_Z + 8
SIDES = 8


def passed_along(value, axis, steps):
    count = lax.axis_size(axis)
    return lax.ppermute(value, axis, [(source, (source + steps) % count) for source in range(count)])


def dispatch_kernel(ids_ref, count_ref, offset_hbm, frac_hbm, normal_hbm, weight_hbm, out_hbm, *scratch):
    offset_ref, frac_ref, normal_ref, weight_ref, out_ref, seen_ref, slot_ref, sems = scratch
    tiles, slots = ids_ref.shape[0], out_hbm.shape[0]
    pairs = ((offset_hbm, offset_ref), (frac_hbm, frac_ref), (normal_hbm, normal_ref), (weight_hbm, weight_ref))
    loads = [pltpu.make_async_copy(source, target, sems.at[i]) for i, (source, target) in enumerate(pairs)]
    for load in loads:
        load.start()

    def reset(i, _):
        seen_ref[i] = 0
        return 0

    lax.fori_loop(0, seen_ref.shape[0], reset, 0, unroll=16)

    def choose(i, _):
        for j in range(8):
            t = 8 * i + j
            brick = ids_ref[t]
            rank = seen_ref[brick]
            seen_ref[brick] = rank + 1
            slot_ref[t] = jnp.where(t < count_ref[0], brick * CAP + jnp.minimum(rank, CAP - 1), slots)
            out_ref[pl.ds(2 * t, 2)] = jnp.zeros((2,) + out_ref.shape[1:], jnp.float32)
        return 0

    lax.fori_loop(0, tiles // 8, choose, 0)
    for load in loads:
        load.wait()

    def place(i, _):
        here = pl.ds(pl.multiple_of(8 * i, 8), 8)
        rows = [frac_ref[k, here, :] for k in range(3)] + [offset_ref[here, :].astype(jnp.float32)]
        rows += [normal_ref[k, here, :] for k in range(3)] + [weight_ref[here, :]]
        for j in range(8):
            slot = slot_ref[8 * i + j]
            for half in range(out_ref.shape[1] // 8):
                for k, row in enumerate(rows):
                    piece = row[j : j + 1, LANES * half : LANES * half + LANES]
                    out_ref[slot, 8 * half + k : 8 * half + k + 1, :] = piece
        return 0

    lax.fori_loop(0, tiles // 8, place, 0)
    store = pltpu.make_async_copy(out_ref.at[pl.ds(0, slots)], out_hbm, sems.at[len(pairs)])
    store.start()
    store.wait()


def dispatch(ids, count, offset, frac, normal, weight, bricks):
    smem = pl.BlockSpec(memory_space=pltpu.SMEM)
    hbm = pl.BlockSpec(memory_space=pltpu.HBM)
    block = (8 * offset.shape[1] // LANES, LANES)
    slots = bricks * CAP
    return pl.pallas_call(
        dispatch_kernel,
        out_shape=jax.ShapeDtypeStruct((slots,) + block, jnp.float32),
        in_specs=[smem, smem, hbm, hbm, hbm, hbm],
        out_specs=hbm,
        scratch_shapes=[
            pltpu.VMEM(offset.shape, jnp.int32),
            pltpu.VMEM(frac.shape, jnp.float32),
            pltpu.VMEM(normal.shape, jnp.float32),
            pltpu.VMEM(weight.shape, jnp.float32),
            pltpu.VMEM((slots + 1,) + block, jnp.float32),
            pltpu.SMEM((bricks,), jnp.int32),
            pltpu.SMEM(ids.shape, jnp.int32),
            pltpu.SemaphoreType.DMA((5,)),
        ],
        name="dispatch",
    )(ids, count, offset, frac, normal, weight)


def spline(f):
    return (
        [0.5 * (1.0 - f) * (1.0 - f), 0.75 - (f - 0.5) * (f - 0.5), 0.5 * f * f],
        [f - 1.0, 1.0 - 2.0 * f, f],
    )


def spread(cell, cells, pieces):
    here = [cell == c for c in range(cells)]
    out = []
    for target in range(cells + 2):
        value = None
        for i in range(3):
            c = target - i
            if 0 <= c < cells:
                value = jnp.where(here[c], pieces[i], 0.0 if value is None else value)
        out.append(value)
    return out


def prepare(inbox_ref, first, row_ref, side_ref):
    def channel(c):
        return inbox_ref[pl.ds(first * 8 + c, GROUP, stride=8), :]

    offset = channel(3).astype(jnp.int32)
    weights, slopes = spline(channel(0))
    cell = lax.shift_right_logical(offset, 10)
    x_value, x_slope = spread(cell, BX, weights), spread(cell, BX, slopes)
    weights, slopes = spline(channel(1))
    cell = lax.shift_right_logical(offset, 7) & 7
    y_value, y_slope = spread(cell, BY, weights), spread(cell, BY, slopes)
    nx, ny, nz, weight = [channel(c) for c in (4, 5, 6, 7)]
    for r in range(BX + 2):
        parts = (nx * x_slope[r], ny * x_value[r], nz * x_value[r], weight * x_value[r])
        for i, part in enumerate(parts):
            row_ref[ROW_X + 4 * r + i] = part
        for e in range(2):
            yv, ys = y_value[BY + e], y_slope[BY + e]
            ends = (parts[0] * yv + parts[1] * ys, parts[2] * yv, parts[3] * yv)
            for k in range(3):
                side_ref[2 * k + e, GROUP * r : GROUP * r + GROUP, :] = ends[k]
    for s in range(BY):
        side_ref[6, GROUP * s : GROUP * s + GROUP, :] = y_value[s]
        side_ref[7, GROUP * s : GROUP * s + GROUP, :] = y_slope[s]
    weights, slopes = spline(channel(2))
    cell = offset & 127
    rows = weights + slopes + [(cell & 15).astype(jnp.float32), lax.shift_right_logical(cell, 4).astype(jnp.float32)]
    for i, row in enumerate(rows):
        row_ref[ROW_Z + i] = row


def build(row_ref, side_ref, unit):
    def row(i):
        return jnp.broadcast_to(row_ref[i, unit : unit + 1, :], (8, LANES))

    def paired(i):
        v = row(i)
        return jnp.concatenate([v, v], axis=0).astype(jnp.bfloat16)

    def side(i):
        return side_ref[i, pl.ds(unit, 8, stride=GROUP), :]

    y_value, y_slope = side(6), side(7)
    left = [[], [], []]
    for pair in range((BX + 2) // 2):
        blocks = []
        for r in (2 * pair, 2 * pair + 1):
            one, two, three, screen = [row(ROW_X + 4 * r + i) for i in range(4)]
            blocks.append((one * y_value + two * y_slope, three * y_value, screen * y_value))
        for k in range(3):
            left[k].append(jnp.concatenate([blocks[0][k], blocks[1][k]], axis=0).astype(jnp.bfloat16))
    for k in range(3):
        left[k].append(jnp.concatenate([side(2 * k), side(2 * k + 1)], axis=0).astype(jnp.bfloat16))

    depth = lax.broadcasted_iota(jnp.int32, (16, LANES), 0)
    zero = jnp.zeros((16, LANES), jnp.bfloat16)

    def constant(v):
        return v.astype(jnp.float32).astype(jnp.bfloat16)

    low, block_of = paired(ROW_Z + 6), paired(ROW_Z + 7)
    w = [paired(ROW_Z + i) for i in range(6)]
    below = constant((depth + 1) & 15) == low
    value, slope = jnp.where(below, w[0], zero), jnp.where(below, w[3], zero)
    carry = jnp.where(below, constant(jnp.where(depth == 15, -1, 0)), zero)
    same = constant(depth) == low
    value, slope = jnp.where(same, w[1], value), jnp.where(same, w[4], slope)
    above = constant((depth + 15) & 15) == low
    value, slope = jnp.where(above, w[2], value), jnp.where(above, w[5], slope)
    home = block_of + jnp.where(above, constant(jnp.where(depth == 0, 1, 0)), carry)
    right = [[], []]
    for block in range(BZ // 16):
        inside = home == jnp.full((16, LANES), block, jnp.bfloat16)
        right[0].append(jnp.where(inside, value, zero))
        right[1].append(jnp.where(inside, slope, zero))
    return jnp.concatenate(sum(left, []), axis=0), jnp.concatenate(sum(right, []), axis=0)


def splat_kernel(inbox_ref, field_ref, up_ref, down_ref, right_ref, left_ref, acc_ref, row_ref, side_ref):
    batch = GROUP * UNROLL
    steps = inbox_ref.shape[0] // (8 * batch)

    acc_ref[...] = jnp.zeros_like(acc_ref)

    for u in range(UNROLL):
        prepare(inbox_ref, u * GROUP, row_ref.at[u], side_ref.at[u])

    def body(i, _):
        acc = acc_ref[...]
        coming = jnp.minimum(i + 1, steps - 1) * batch
        for u in range(UNROLL):
            for pair in range(GROUP // 2):
                sides = [build(row_ref.at[u], side_ref.at[u], k) for k in (2 * pair, 2 * pair + 1)]
                acc = acc + lax.dot_general(
                    jnp.concatenate([a for a, _ in sides], axis=1),
                    jnp.concatenate([z for _, z in sides], axis=1),
                    (((1,), (1,)), ((), ())),
                    preferred_element_type=jnp.float32,
                )
            prepare(inbox_ref, coming + u * GROUP, row_ref.at[u], side_ref.at[u])
        acc_ref[...] = acc
        return 0

    lax.fori_loop(0, steps, body, 0)
    for k in range(2):
        first = 2 * ROWS * k
        if k == 0:
            acc_ref[0:ROWS, 0:BZ] = acc_ref[0:ROWS, 0:BZ] + acc_ref[ROWS : 2 * ROWS, BZ : 2 * BZ]

        def rows(at, count, first=first):
            return acc_ref[first + at : first + at + count, 0:BZ]

        for r in range(BX):
            field_ref[k, r, 0 : BY - 1, :] = rows(BY * (r + 1) + 1, BY - 1)
            field_ref[k, r, BY - 1 : BY, :] = rows(PLANES + r + 1, 1)
            left_ref[BX * k + r : BX * k + r + 1, :] = rows(BY * (r + 1), 1)
        right_ref[BX * k : BX * k + BX, :] = rows(PLANES + 9, BX)
        for ref, r in ((up_ref, BX + 1), (down_ref, 0)):
            ref[BY * k : BY * k + BY - 1, :] = rows(BY * r + 1, BY - 1)
            ref[BY * k + BY - 1 : BY * k + BY, :] = rows(PLANES + r, 1)
            ref[16 + k : 17 + k, :] = rows(BY * r, 1)
            ref[18 + k : 19 + k, :] = rows(PLANES + 8 + r, 1)
    for ref in (up_ref, down_ref):
        ref[20:24, :] = jnp.zeros((4, BZ), jnp.float32)


def splat(inbox):
    vmem = pl.BlockSpec(memory_space=pltpu.VMEM)
    shapes = ((2, BX, BY, BZ), (24, BZ), (24, BZ), (2 * BX, BZ), (2 * BX, BZ))
    return pl.pallas_call(
        splat_kernel,
        out_shape=tuple(jax.ShapeDtypeStruct(shape, jnp.float32) for shape in shapes),
        in_specs=[vmem],
        out_specs=(vmem,) * len(shapes),
        scratch_shapes=[
            pltpu.VMEM((3 * ROWS, 2 * BZ), jnp.float32),
            pltpu.VMEM((UNROLL, ROW_COUNT, GROUP, LANES), jnp.float32),
            pltpu.VMEM((UNROLL, SIDES, 8 * GROUP, LANES), jnp.float32),
        ],
        compiler_params=pltpu.CompilerParams(vmem_limit_bytes=16 * 1024 * 1024),
        name="splat",
    )(inbox)


def join_kernel(edge_ref, below_ref, above_ref, right_ref, left_ref, right_out, left_out):
    below = jnp.where(edge_ref[0] == 0, 0.0, below_ref[16:24, :])
    above = jnp.where(edge_ref[1] == 0, 0.0, above_ref[16:24, :])
    right_out[...] = right_ref[...]
    left_out[...] = left_ref[...]
    for k in range(2):
        for out, at in ((left_out, k), (right_out, 2 + k)):
            first, last = BX * k, BX * k + BX - 1
            out[first : first + 1, :] = out[first : first + 1, :] + below[at : at + 1]
            out[last : last + 1, :] = out[last : last + 1, :] + above[at : at + 1]


def join(edges, below, above, right, left):
    smem = pl.BlockSpec(memory_space=pltpu.SMEM)
    vmem = pl.BlockSpec(memory_space=pltpu.VMEM)
    shape = jax.ShapeDtypeStruct(right.shape, jnp.float32)
    return pl.pallas_call(
        join_kernel,
        out_shape=(shape, shape),
        in_specs=[smem] + [vmem] * 4,
        out_specs=(vmem, vmem),
        compiler_params=pltpu.CompilerParams(vmem_limit_bytes=4 * 1024 * 1024),
        name="join",
    )(edges, below, above, right, left)


def finish_kernel(edge_ref, field_ref, below_ref, above_ref, before_ref, after_ref, rhs_ref, screen_ref):
    for k, ref in enumerate((rhs_ref, screen_ref)):
        for r in range(BX):
            plane = field_ref[k, r]
            if r == 0:
                plane = plane + jnp.where(edge_ref[0] == 0, 0.0, below_ref[BY * k : BY * k + BY, :])
            if r == BX - 1:
                plane = plane + jnp.where(edge_ref[1] == 0, 0.0, above_ref[BY * k : BY * k + BY, :])
            ref[r] = plane
            at = BX * k + r
            before = jnp.where(edge_ref[2] == 0, 0.0, before_ref[at : at + 1, :])
            after = jnp.where(edge_ref[3] == 0, 0.0, after_ref[at : at + 1, :])
            ref[r, 0:1, :] = ref[r, 0:1, :] + before
            ref[r, BY - 1 : BY, :] = ref[r, BY - 1 : BY, :] + after


def finish(edges, field, below, above, before, after):
    smem = pl.BlockSpec(memory_space=pltpu.SMEM)
    vmem = pl.BlockSpec(memory_space=pltpu.VMEM)
    shape = jax.ShapeDtypeStruct((BX, BY, BZ), jnp.float32)
    return pl.pallas_call(
        finish_kernel,
        out_shape=(shape, shape),
        in_specs=[smem] + [vmem] * 5,
        out_specs=(vmem, vmem),
        compiler_params=pltpu.CompilerParams(vmem_limit_bytes=4 * 1024 * 1024),
        name="finish",
    )(edges, field, below, above, before, after)


def shards(brick_ids, voxel_offset, fractions, normals, point_weight, tile_count):
    slabs, columns = lax.axis_size("gx"), lax.axis_size("yz")
    outbox = dispatch(
        brick_ids[:, 0],
        tile_count,
        voxel_offset,
        jnp.transpose(fractions, (1, 0, 2)),
        jnp.transpose(normals, (1, 0, 2)),
        point_weight,
        slabs * columns,
    )
    inbox = lax.all_to_all(outbox, ("gx", "yz"), split_axis=0, concat_axis=0, tiled=True)
    slab, column = lax.axis_index("gx"), lax.axis_index("yz")
    edges = jnp.stack([slab, slabs - 1 - slab, column, columns - 1 - column])
    field, up, down, right, left = splat(inbox.reshape(-1, LANES))
    below = passed_along(up, "gx", 1)
    above = passed_along(down, "gx", -1)
    right, left = join(edges, below, above, right, left)
    before = passed_along(right, "yz", 1)
    after = passed_along(left, "yz", -1)
    return finish(edges, field, below, above, before, after)


def solution(mesh):
    return jax.shard_map(
        shards,
        mesh=mesh,
        in_specs=(
            P(("gx", "yz"), None),
            P(("gx", "yz"), None),
            P(("gx", "yz"), None, None),
            P(("gx", "yz"), None, None),
            P(("gx", "yz"), None),
            P(("gx", "yz")),
        ),
        out_specs=(P("gx", "yz", None), P("gx", "yz", None)),
        check_vma=False,
    )
```

```python
import jax
import jax.numpy as jnp
from jax import lax
from jax.experimental import pallas as pl
from jax.experimental.pallas import tpu as pltpu
from jax.sharding import PartitionSpec as P

BX = 4
BY = 8
BZ = 128
CAP = 2
LANES = 128
GROUP = 8
UNROLL = 16
AHEAD = 2
SLOTS = 16
PLANES = (BX + 2) * BY
ENDS = 16
ROWS = PLANES + ENDS
ROW_X = 0
ROW_Z = 4 * (BX + 2)
ROW_COUNT = ROW_Z + 8
SIDES = 8


def passed_along(value, axis, steps):
    count = lax.axis_size(axis)
    return lax.ppermute(value, axis, [(source, (source + steps) % count) for source in range(count)])


def dispatch_kernel(ids_ref, count_ref, offset_hbm, frac_hbm, normal_hbm, weight_hbm, out_hbm, *scratch):
    offset_ref, frac_ref, normal_ref, weight_ref, out_ref, seen_ref, slot_ref, sems = scratch
    tiles, slots = ids_ref.shape[0], out_hbm.shape[0]
    pairs = ((offset_hbm, offset_ref), (frac_hbm, frac_ref), (normal_hbm, normal_ref), (weight_hbm, weight_ref))
    loads = [pltpu.make_async_copy(source, target, sems.at[i]) for i, (source, target) in enumerate(pairs)]
    for load in loads:
        load.start()

    def reset(i, _):
        seen_ref[i] = 0
        return 0

    lax.fori_loop(0, seen_ref.shape[0], reset, 0, unroll=16)

    def choose(i, _):
        for j in range(8):
            t = 8 * i + j
            brick = ids_ref[t]
            rank = seen_ref[brick]
            seen_ref[brick] = rank + 1
            slot_ref[t] = jnp.where(t < count_ref[0], brick * CAP + jnp.minimum(rank, CAP - 1), slots)
            out_ref[pl.ds(2 * t, 2)] = jnp.zeros((2,) + out_ref.shape[1:], jnp.float32)
        return 0

    lax.fori_loop(0, tiles // 8, choose, 0)
    for load in loads:
        load.wait()

    def place(i, _):
        here = pl.ds(pl.multiple_of(8 * i, 8), 8)
        rows = [frac_ref[k, here, :] for k in range(3)] + [offset_ref[here, :].astype(jnp.float32)]
        rows += [normal_ref[k, here, :] for k in range(3)] + [weight_ref[here, :]]
        for j in range(8):
            slot = slot_ref[8 * i + j]
            for half in range(out_ref.shape[1] // 8):
                for k, row in enumerate(rows):
                    piece = row[j : j + 1, LANES * half : LANES * half + LANES]
                    out_ref[slot, 8 * half + k : 8 * half + k + 1, :] = piece
        return 0

    lax.fori_loop(0, tiles // 8, place, 0)
    store = pltpu.make_async_copy(out_ref.at[pl.ds(0, slots)], out_hbm, sems.at[len(pairs)])
    store.start()
    store.wait()


def dispatch(ids, count, offset, frac, normal, weight, bricks):
    smem = pl.BlockSpec(memory_space=pltpu.SMEM)
    hbm = pl.BlockSpec(memory_space=pltpu.HBM)
    block = (8 * offset.shape[1] // LANES, LANES)
    slots = bricks * CAP
    return pl.pallas_call(
        dispatch_kernel,
        out_shape=jax.ShapeDtypeStruct((slots,) + block, jnp.float32),
        in_specs=[smem, smem, hbm, hbm, hbm, hbm],
        out_specs=hbm,
        scratch_shapes=[
            pltpu.VMEM(offset.shape, jnp.int32),
            pltpu.VMEM(frac.shape, jnp.float32),
            pltpu.VMEM(normal.shape, jnp.float32),
            pltpu.VMEM(weight.shape, jnp.float32),
            pltpu.VMEM((slots + 1,) + block, jnp.float32),
            pltpu.SMEM((bricks,), jnp.int32),
            pltpu.SMEM(ids.shape, jnp.int32),
            pltpu.SemaphoreType.DMA((5,)),
        ],
        name="dispatch",
    )(ids, count, offset, frac, normal, weight)


def spline(f):
    return (
        [0.5 * (1.0 - f) * (1.0 - f), 0.75 - (f - 0.5) * (f - 0.5), 0.5 * f * f],
        [f - 1.0, 1.0 - 2.0 * f, f],
    )


def spread(cell, cells, pieces):
    here = [cell == c for c in range(cells)]
    out = []
    for target in range(cells + 2):
        value = None
        for i in range(3):
            c = target - i
            if 0 <= c < cells:
                value = jnp.where(here[c], pieces[i], 0.0 if value is None else value)
        out.append(value)
    return out


def prepare(inbox_ref, first, row_ref, side_ref):
    def channel(c):
        return inbox_ref[pl.ds(first * 8 + c, GROUP, stride=8), :]

    def put(i, s, v):
        for h in range(2):
            side_ref[i, h, 4 * s : 4 * s + 4, :] = v[4 * h : 4 * h + 4]

    offset = channel(3).astype(jnp.int32)
    weights, slopes = spline(channel(0))
    cell = lax.shift_right_logical(offset, 10)
    x_value, x_slope = spread(cell, BX, weights), spread(cell, BX, slopes)
    weights, slopes = spline(channel(1))
    cell = lax.shift_right_logical(offset, 7) & 7
    y_value, y_slope = spread(cell, BY, weights), spread(cell, BY, slopes)
    nx, ny, nz, weight = [channel(c) for c in (4, 5, 6, 7)]
    for r in range(BX + 2):
        parts = (nx * x_slope[r], ny * x_value[r], nz * x_value[r], weight * x_value[r])
        for i, part in enumerate(parts):
            row_ref[ROW_X + 4 * r + i] = part
        for e in range(2):
            yv, ys = y_value[BY + e], y_slope[BY + e]
            ends = (parts[0] * yv + parts[1] * ys, parts[2] * yv, parts[3] * yv)
            for k in range(3):
                put(2 * k + e, r, ends[k])
    for s in range(BY):
        put(6, s, y_value[s])
        put(7, s, y_slope[s])
    weights, slopes = spline(channel(2))
    cell = offset & 127
    rows = weights + slopes + [(cell & 15).astype(jnp.float32), lax.shift_right_logical(cell, 4).astype(jnp.float32)]
    for i, row in enumerate(rows):
        row_ref[ROW_Z + i] = row


def build(row_ref, side_ref, unit):
    def row(i):
        return jnp.broadcast_to(row_ref[i, unit : unit + 1, :], (8, LANES))

    def paired(i):
        v = row(i)
        return jnp.concatenate([v, v], axis=0).astype(jnp.bfloat16)

    def side(i):
        return side_ref[i, unit // 4, pl.ds(unit % 4, 8, stride=4), :]

    y_value, y_slope = side(6), side(7)
    left = [[], [], []]
    for pair in range((BX + 2) // 2):
        blocks = []
        for r in (2 * pair, 2 * pair + 1):
            one, two, three, screen = [row(ROW_X + 4 * r + i) for i in range(4)]
            blocks.append((one * y_value + two * y_slope, three * y_value, screen * y_value))
        for k in range(3):
            left[k].append(jnp.concatenate([blocks[0][k], blocks[1][k]], axis=0).astype(jnp.bfloat16))
    for k in range(3):
        left[k].append(jnp.concatenate([side(2 * k), side(2 * k + 1)], axis=0).astype(jnp.bfloat16))

    depth = lax.broadcasted_iota(jnp.int32, (16, LANES), 0)
    zero = jnp.zeros((16, LANES), jnp.bfloat16)

    def constant(v):
        return v.astype(jnp.float32).astype(jnp.bfloat16)

    low, block_of = paired(ROW_Z + 6), paired(ROW_Z + 7)
    w = [paired(ROW_Z + i) for i in range(6)]
    below = constant((depth + 1) & 15) == low
    value, slope = jnp.where(below, w[0], zero), jnp.where(below, w[3], zero)
    carry = jnp.where(below, constant(jnp.where(depth == 15, -1, 0)), zero)
    same = constant(depth) == low
    value, slope = jnp.where(same, w[1], value), jnp.where(same, w[4], slope)
    above = constant((depth + 15) & 15) == low
    value, slope = jnp.where(above, w[2], value), jnp.where(above, w[5], slope)
    home = block_of + jnp.where(above, constant(jnp.where(depth == 0, 1, 0)), carry)
    right = [[], []]
    for block in range(BZ // 16):
        inside = home == jnp.full((16, LANES), block, jnp.bfloat16)
        right[0].append(jnp.where(inside, value, zero))
        right[1].append(jnp.where(inside, slope, zero))
    return jnp.concatenate(sum(left, []), axis=0), jnp.concatenate(sum(right, []), axis=0)


def splat_kernel(inbox_ref, field_ref, up_ref, down_ref, right_ref, left_ref, acc_ref, row_ref, side_ref):
    batch = GROUP * UNROLL
    steps = inbox_ref.shape[0] // (8 * batch)

    acc_ref[...] = jnp.zeros_like(acc_ref)

    def ready(group, slot):
        group = jnp.minimum(group, steps * UNROLL - 1)
        prepare(inbox_ref, group * GROUP, row_ref.at[slot], side_ref.at[slot])

    for u in range(AHEAD):
        ready(u, u)

    def body(i, _):
        acc = acc_ref[...]
        for u in range(UNROLL):
            slot = u % SLOTS
            for pair in range(GROUP // 2):
                sides = [build(row_ref.at[slot], side_ref.at[slot], k) for k in (2 * pair, 2 * pair + 1)]
                acc = acc + lax.dot_general(
                    jnp.concatenate([a for a, _ in sides], axis=1),
                    jnp.concatenate([z for _, z in sides], axis=1),
                    (((1,), (1,)), ((), ())),
                    preferred_element_type=jnp.float32,
                )
            ready(i * UNROLL + u + AHEAD, (u + AHEAD) % SLOTS)
        acc_ref[...] = acc
        return 0

    lax.fori_loop(0, steps, body, 0)
    for k in range(2):
        first = 2 * ROWS * k
        if k == 0:
            acc_ref[0:ROWS, 0:BZ] = acc_ref[0:ROWS, 0:BZ] + acc_ref[ROWS : 2 * ROWS, BZ : 2 * BZ]

        def rows(at, count, first=first):
            return acc_ref[first + at : first + at + count, 0:BZ]

        for r in range(BX):
            field_ref[k, r, 0 : BY - 1, :] = rows(BY * (r + 1) + 1, BY - 1)
            field_ref[k, r, BY - 1 : BY, :] = rows(PLANES + r + 1, 1)
            left_ref[BX * k + r : BX * k + r + 1, :] = rows(BY * (r + 1), 1)
        right_ref[BX * k : BX * k + BX, :] = rows(PLANES + 9, BX)
        for ref, r in ((up_ref, BX + 1), (down_ref, 0)):
            ref[BY * k : BY * k + BY - 1, :] = rows(BY * r + 1, BY - 1)
            ref[BY * k + BY - 1 : BY * k + BY, :] = rows(PLANES + r, 1)
            ref[16 + k : 17 + k, :] = rows(BY * r, 1)
            ref[18 + k : 19 + k, :] = rows(PLANES + 8 + r, 1)
    for ref in (up_ref, down_ref):
        ref[20:24, :] = jnp.zeros((4, BZ), jnp.float32)


def splat(inbox):
    vmem = pl.BlockSpec(memory_space=pltpu.VMEM)
    shapes = ((2, BX, BY, BZ), (24, BZ), (24, BZ), (2 * BX, BZ), (2 * BX, BZ))
    return pl.pallas_call(
        splat_kernel,
        out_shape=tuple(jax.ShapeDtypeStruct(shape, jnp.float32) for shape in shapes),
        in_specs=[vmem],
        out_specs=(vmem,) * len(shapes),
        scratch_shapes=[
            pltpu.VMEM((3 * ROWS, 2 * BZ), jnp.float32),
            pltpu.VMEM((SLOTS, ROW_COUNT, GROUP, LANES), jnp.float32),
            pltpu.VMEM((SLOTS, SIDES, 2, 4 * 8, LANES), jnp.float32),
        ],
        compiler_params=pltpu.CompilerParams(vmem_limit_bytes=16 * 1024 * 1024),
        name="splat",
    )(inbox)


def join_kernel(edge_ref, below_ref, above_ref, right_ref, left_ref, right_out, left_out):
    below = jnp.where(edge_ref[0] == 0, 0.0, below_ref[16:24, :])
    above = jnp.where(edge_ref[1] == 0, 0.0, above_ref[16:24, :])
    right_out[...] = right_ref[...]
    left_out[...] = left_ref[...]
    for k in range(2):
        for out, at in ((left_out, k), (right_out, 2 + k)):
            first, last = BX * k, BX * k + BX - 1
            out[first : first + 1, :] = out[first : first + 1, :] + below[at : at + 1]
            out[last : last + 1, :] = out[last : last + 1, :] + above[at : at + 1]


def join(edges, below, above, right, left):
    smem = pl.BlockSpec(memory_space=pltpu.SMEM)
    vmem = pl.BlockSpec(memory_space=pltpu.VMEM)
    shape = jax.ShapeDtypeStruct(right.shape, jnp.float32)
    return pl.pallas_call(
        join_kernel,
        out_shape=(shape, shape),
        in_specs=[smem] + [vmem] * 4,
        out_specs=(vmem, vmem),
        compiler_params=pltpu.CompilerParams(vmem_limit_bytes=4 * 1024 * 1024),
        name="join",
    )(edges, below, above, right, left)


def finish_kernel(edge_ref, field_ref, below_ref, above_ref, before_ref, after_ref, rhs_ref, screen_ref):
    for k, ref in enumerate((rhs_ref, screen_ref)):
        for r in range(BX):
            plane = field_ref[k, r]
            if r == 0:
                plane = plane + jnp.where(edge_ref[0] == 0, 0.0, below_ref[BY * k : BY * k + BY, :])
            if r == BX - 1:
                plane = plane + jnp.where(edge_ref[1] == 0, 0.0, above_ref[BY * k : BY * k + BY, :])
            ref[r] = plane
            at = BX * k + r
            before = jnp.where(edge_ref[2] == 0, 0.0, before_ref[at : at + 1, :])
            after = jnp.where(edge_ref[3] == 0, 0.0, after_ref[at : at + 1, :])
            ref[r, 0:1, :] = ref[r, 0:1, :] + before
            ref[r, BY - 1 : BY, :] = ref[r, BY - 1 : BY, :] + after


def finish(edges, field, below, above, before, after):
    smem = pl.BlockSpec(memory_space=pltpu.SMEM)
    vmem = pl.BlockSpec(memory_space=pltpu.VMEM)
    shape = jax.ShapeDtypeStruct((BX, BY, BZ), jnp.float32)
    return pl.pallas_call(
        finish_kernel,
        out_shape=(shape, shape),
        in_specs=[smem] + [vmem] * 5,
        out_specs=(vmem, vmem),
        compiler_params=pltpu.CompilerParams(vmem_limit_bytes=4 * 1024 * 1024),
        name="finish",
    )(edges, field, below, above, before, after)


def shards(brick_ids, voxel_offset, fractions, normals, point_weight, tile_count):
    slabs, columns = lax.axis_size("gx"), lax.axis_size("yz")
    outbox = dispatch(
        brick_ids[:, 0],
        tile_count,
        voxel_offset,
        jnp.transpose(fractions, (1, 0, 2)),
        jnp.transpose(normals, (1, 0, 2)),
        point_weight,
        slabs * columns,
    )
    inbox = lax.all_to_all(outbox, ("gx", "yz"), split_axis=0, concat_axis=0, tiled=True)
    slab, column = lax.axis_index("gx"), lax.axis_index("yz")
    edges = jnp.stack([slab, slabs - 1 - slab, column, columns - 1 - column])
    field, up, down, right, left = splat(inbox.reshape(-1, LANES))
    below = passed_along(up, "gx", 1)
    above = passed_along(down, "gx", -1)
    right, left = join(edges, below, above, right, left)
    before = passed_along(right, "yz", 1)
    after = passed_along(left, "yz", -1)
    return finish(edges, field, below, above, before, after)


def solution(mesh):
    return jax.shard_map(
        shards,
        mesh=mesh,
        in_specs=(
            P(("gx", "yz"), None),
            P(("gx", "yz"), None),
            P(("gx", "yz"), None, None),
            P(("gx", "yz"), None, None),
            P(("gx", "yz"), None),
            P(("gx", "yz")),
        ),
        out_specs=(P("gx", "yz", None), P("gx", "yz", None)),
        check_vma=False,
    )
```

```python
import jax
import jax.numpy as jnp
from jax import lax
from jax.experimental import pallas as pl
from jax.experimental.pallas import tpu as pltpu
from jax.sharding import PartitionSpec as P

BX = 4
BY = 8
BZ = 128
CAP = 2
LANES = 128
GROUP = 8
UNROLL = 32
AHEAD = 1
SLOTS = 32
PLANES = (BX + 2) * BY
ENDS = 16
ROWS = PLANES + ENDS
ROW_X = 0
ROW_Z = 4 * (BX + 2)
ROW_COUNT = ROW_Z + 8
SIDES = 8


def passed_along(value, axis, steps):
    count = lax.axis_size(axis)
    return lax.ppermute(value, axis, [(source, (source + steps) % count) for source in range(count)])


def dispatch_kernel(ids_ref, count_ref, offset_hbm, frac_hbm, normal_hbm, weight_hbm, out_hbm, *scratch):
    offset_ref, frac_ref, normal_ref, weight_ref, out_ref, seen_ref, slot_ref, sems = scratch
    tiles, slots = ids_ref.shape[0], out_hbm.shape[0]
    pairs = ((offset_hbm, offset_ref), (frac_hbm, frac_ref), (normal_hbm, normal_ref), (weight_hbm, weight_ref))
    loads = [pltpu.make_async_copy(source, target, sems.at[i]) for i, (source, target) in enumerate(pairs)]
    for load in loads:
        load.start()

    def reset(i, _):
        seen_ref[i] = 0
        return 0

    lax.fori_loop(0, seen_ref.shape[0], reset, 0, unroll=16)

    def choose(i, _):
        for j in range(8):
            t = 8 * i + j
            brick = ids_ref[t]
            rank = seen_ref[brick]
            seen_ref[brick] = rank + 1
            slot_ref[t] = jnp.where(t < count_ref[0], brick * CAP + jnp.minimum(rank, CAP - 1), slots)
            out_ref[pl.ds(2 * t, 2)] = jnp.zeros((2,) + out_ref.shape[1:], jnp.float32)
        return 0

    lax.fori_loop(0, tiles // 8, choose, 0)
    for load in loads:
        load.wait()

    def place(i, _):
        here = pl.ds(pl.multiple_of(8 * i, 8), 8)
        rows = [frac_ref[k, here, :] for k in range(3)] + [offset_ref[here, :].astype(jnp.float32)]
        rows += [normal_ref[k, here, :] for k in range(3)] + [weight_ref[here, :]]
        for j in range(8):
            slot = slot_ref[8 * i + j]
            for half in range(out_ref.shape[1] // 8):
                for k, row in enumerate(rows):
                    piece = row[j : j + 1, LANES * half : LANES * half + LANES]
                    out_ref[slot, 8 * half + k : 8 * half + k + 1, :] = piece
        return 0

    lax.fori_loop(0, tiles // 8, place, 0)
    store = pltpu.make_async_copy(out_ref.at[pl.ds(0, slots)], out_hbm, sems.at[len(pairs)])
    store.start()
    store.wait()


def dispatch(ids, count, offset, frac, normal, weight, bricks):
    smem = pl.BlockSpec(memory_space=pltpu.SMEM)
    hbm = pl.BlockSpec(memory_space=pltpu.HBM)
    block = (8 * offset.shape[1] // LANES, LANES)
    slots = bricks * CAP
    return pl.pallas_call(
        dispatch_kernel,
        out_shape=jax.ShapeDtypeStruct((slots,) + block, jnp.float32),
        in_specs=[smem, smem, hbm, hbm, hbm, hbm],
        out_specs=hbm,
        scratch_shapes=[
            pltpu.VMEM(offset.shape, jnp.int32),
            pltpu.VMEM(frac.shape, jnp.float32),
            pltpu.VMEM(normal.shape, jnp.float32),
            pltpu.VMEM(weight.shape, jnp.float32),
            pltpu.VMEM((slots + 1,) + block, jnp.float32),
            pltpu.SMEM((bricks,), jnp.int32),
            pltpu.SMEM(ids.shape, jnp.int32),
            pltpu.SemaphoreType.DMA((5,)),
        ],
        name="dispatch",
    )(ids, count, offset, frac, normal, weight)


def spline(f):
    return (
        [0.5 * (1.0 - f) * (1.0 - f), 0.75 - (f - 0.5) * (f - 0.5), 0.5 * f * f],
        [f - 1.0, 1.0 - 2.0 * f, f],
    )


def spread(cell, cells, pieces):
    here = [cell == c for c in range(cells)]
    out = []
    for target in range(cells + 2):
        value = None
        for i in range(3):
            c = target - i
            if 0 <= c < cells:
                value = jnp.where(here[c], pieces[i], 0.0 if value is None else value)
        out.append(value)
    return out


def prepare(inbox_ref, first, row_ref, side_ref):
    def channel(c):
        return inbox_ref[pl.ds(first * 8 + c, GROUP, stride=8), :]

    def put(i, s, v):
        for h in range(2):
            side_ref[i, h, 4 * s : 4 * s + 4, :] = v[4 * h : 4 * h + 4]

    offset = channel(3).astype(jnp.int32)
    weights, slopes = spline(channel(0))
    cell = lax.shift_right_logical(offset, 10)
    x_value, x_slope = spread(cell, BX, weights), spread(cell, BX, slopes)
    weights, slopes = spline(channel(1))
    cell = lax.shift_right_logical(offset, 7) & 7
    y_value, y_slope = spread(cell, BY, weights), spread(cell, BY, slopes)
    nx, ny, nz, weight = [channel(c) for c in (4, 5, 6, 7)]
    for r in range(BX + 2):
        parts = (nx * x_slope[r], ny * x_value[r], nz * x_value[r], weight * x_value[r])
        for i, part in enumerate(parts):
            row_ref[ROW_X + 4 * r + i] = part
        for e in range(2):
            yv, ys = y_value[BY + e], y_slope[BY + e]
            ends = (parts[0] * yv + parts[1] * ys, parts[2] * yv, parts[3] * yv)
            for k in range(3):
                put(2 * k + e, r, ends[k])
    for s in range(BY):
        put(6, s, y_value[s])
        put(7, s, y_slope[s])
    weights, slopes = spline(channel(2))
    cell = offset & 127
    rows = weights + slopes + [(cell & 15).astype(jnp.float32), lax.shift_right_logical(cell, 4).astype(jnp.float32)]
    for i, row in enumerate(rows):
        row_ref[ROW_Z + i] = row


def build(row_ref, side_ref, unit):
    def row(i):
        return jnp.broadcast_to(row_ref[i, unit : unit + 1, :], (8, LANES))

    def paired(i):
        v = row(i)
        return jnp.concatenate([v, v], axis=0).astype(jnp.bfloat16)

    def side(i):
        return side_ref[i, unit // 4, pl.ds(unit % 4, 8, stride=4), :]

    y_value, y_slope = side(6), side(7)
    left = [[], [], []]
    for pair in range((BX + 2) // 2):
        blocks = []
        for r in (2 * pair, 2 * pair + 1):
            one, two, three, screen = [row(ROW_X + 4 * r + i) for i in range(4)]
            blocks.append((one * y_value + two * y_slope, three * y_value, screen * y_value))
        for k in range(3):
            left[k].append(jnp.concatenate([blocks[0][k], blocks[1][k]], axis=0).astype(jnp.bfloat16))
    for k in range(3):
        left[k].append(jnp.concatenate([side(2 * k), side(2 * k + 1)], axis=0).astype(jnp.bfloat16))

    depth = lax.broadcasted_iota(jnp.int32, (16, LANES), 0)
    zero = jnp.zeros((16, LANES), jnp.bfloat16)

    def constant(v):
        return v.astype(jnp.float32).astype(jnp.bfloat16)

    low, block_of = paired(ROW_Z + 6), paired(ROW_Z + 7)
    w = [paired(ROW_Z + i) for i in range(6)]
    below = constant((depth + 1) & 15) == low
    value, slope = jnp.where(below, w[0], zero), jnp.where(below, w[3], zero)
    carry = jnp.where(below, constant(jnp.where(depth == 15, -1, 0)), zero)
    same = constant(depth) == low
    value, slope = jnp.where(same, w[1], value), jnp.where(same, w[4], slope)
    above = constant((depth + 15) & 15) == low
    value, slope = jnp.where(above, w[2], value), jnp.where(above, w[5], slope)
    home = block_of + jnp.where(above, constant(jnp.where(depth == 0, 1, 0)), carry)
    right = [[], []]
    for block in range(BZ // 16):
        inside = home == jnp.full((16, LANES), block, jnp.bfloat16)
        right[0].append(jnp.where(inside, value, zero))
        right[1].append(jnp.where(inside, slope, zero))
    return jnp.concatenate(sum(left, []), axis=0), jnp.concatenate(sum(right, []), axis=0)


def splat_kernel(inbox_ref, field_ref, up_ref, down_ref, right_ref, left_ref, acc_ref, row_ref, side_ref):
    batch = GROUP * UNROLL
    steps = inbox_ref.shape[0] // (8 * batch)

    acc_ref[...] = jnp.zeros_like(acc_ref)

    def ready(group, slot):
        group = jnp.minimum(group, steps * UNROLL - 1)
        prepare(inbox_ref, group * GROUP, row_ref.at[slot], side_ref.at[slot])

    for u in range(AHEAD):
        ready(u, u)

    def body(i, _):
        acc = acc_ref[...]
        for u in range(UNROLL):
            slot = u % SLOTS
            for pair in range(GROUP // 2):
                sides = [build(row_ref.at[slot], side_ref.at[slot], k) for k in (2 * pair, 2 * pair + 1)]
                acc = acc + lax.dot_general(
                    jnp.concatenate([a for a, _ in sides], axis=1),
                    jnp.concatenate([z for _, z in sides], axis=1),
                    (((1,), (1,)), ((), ())),
                    preferred_element_type=jnp.float32,
                )
            ready(i * UNROLL + u + AHEAD, (u + AHEAD) % SLOTS)
        acc_ref[...] = acc
        return 0

    lax.fori_loop(0, steps, body, 0)
    for k in range(2):
        first = 2 * ROWS * k
        if k == 0:
            acc_ref[0:ROWS, 0:BZ] = acc_ref[0:ROWS, 0:BZ] + acc_ref[ROWS : 2 * ROWS, BZ : 2 * BZ]

        def rows(at, count, first=first):
            return acc_ref[first + at : first + at + count, 0:BZ]

        for r in range(BX):
            field_ref[k, r, 0 : BY - 1, :] = rows(BY * (r + 1) + 1, BY - 1)
            field_ref[k, r, BY - 1 : BY, :] = rows(PLANES + r + 1, 1)
            left_ref[BX * k + r : BX * k + r + 1, :] = rows(BY * (r + 1), 1)
        right_ref[BX * k : BX * k + BX, :] = rows(PLANES + 9, BX)
        for ref, r in ((up_ref, BX + 1), (down_ref, 0)):
            ref[BY * k : BY * k + BY - 1, :] = rows(BY * r + 1, BY - 1)
            ref[BY * k + BY - 1 : BY * k + BY, :] = rows(PLANES + r, 1)
            ref[16 + k : 17 + k, :] = rows(BY * r, 1)
            ref[18 + k : 19 + k, :] = rows(PLANES + 8 + r, 1)
    for ref in (up_ref, down_ref):
        ref[20:24, :] = jnp.zeros((4, BZ), jnp.float32)


def splat(inbox):
    vmem = pl.BlockSpec(memory_space=pltpu.VMEM)
    shapes = ((2, BX, BY, BZ), (24, BZ), (24, BZ), (2 * BX, BZ), (2 * BX, BZ))
    return pl.pallas_call(
        splat_kernel,
        out_shape=tuple(jax.ShapeDtypeStruct(shape, jnp.float32) for shape in shapes),
        in_specs=[vmem],
        out_specs=(vmem,) * len(shapes),
        scratch_shapes=[
            pltpu.VMEM((3 * ROWS, 2 * BZ), jnp.float32),
            pltpu.VMEM((SLOTS, ROW_COUNT, GROUP, LANES), jnp.float32),
            pltpu.VMEM((SLOTS, SIDES, 2, 4 * 8, LANES), jnp.float32),
        ],
        compiler_params=pltpu.CompilerParams(vmem_limit_bytes=16 * 1024 * 1024),
        name="splat",
    )(inbox)


def join_kernel(edge_ref, below_ref, above_ref, right_ref, left_ref, right_out, left_out):
    below = jnp.where(edge_ref[0] == 0, 0.0, below_ref[16:24, :])
    above = jnp.where(edge_ref[1] == 0, 0.0, above_ref[16:24, :])
    right_out[...] = right_ref[...]
    left_out[...] = left_ref[...]
    for k in range(2):
        for out, at in ((left_out, k), (right_out, 2 + k)):
            first, last = BX * k, BX * k + BX - 1
            out[first : first + 1, :] = out[first : first + 1, :] + below[at : at + 1]
            out[last : last + 1, :] = out[last : last + 1, :] + above[at : at + 1]


def join(edges, below, above, right, left):
    smem = pl.BlockSpec(memory_space=pltpu.SMEM)
    vmem = pl.BlockSpec(memory_space=pltpu.VMEM)
    shape = jax.ShapeDtypeStruct(right.shape, jnp.float32)
    return pl.pallas_call(
        join_kernel,
        out_shape=(shape, shape),
        in_specs=[smem] + [vmem] * 4,
        out_specs=(vmem, vmem),
        compiler_params=pltpu.CompilerParams(vmem_limit_bytes=4 * 1024 * 1024),
        name="join",
    )(edges, below, above, right, left)


def widen_kernel(edge_ref, field_ref, below_ref, above_ref, out_ref):
    for k in range(2):
        for r in range(BX):
            plane = field_ref[k, r]
            if r == 0:
                plane = plane + jnp.where(edge_ref[0] == 0, 0.0, below_ref[BY * k : BY * k + BY, :])
            if r == BX - 1:
                plane = plane + jnp.where(edge_ref[1] == 0, 0.0, above_ref[BY * k : BY * k + BY, :])
            out_ref[k, r] = plane


def widen(edges, field, below, above):
    smem = pl.BlockSpec(memory_space=pltpu.SMEM)
    vmem = pl.BlockSpec(memory_space=pltpu.VMEM)
    return pl.pallas_call(
        widen_kernel,
        out_shape=jax.ShapeDtypeStruct(field.shape, jnp.float32),
        in_specs=[smem] + [vmem] * 3,
        out_specs=vmem,
        cost_estimate=pl.CostEstimate(flops=20000000, bytes_accessed=100000, transcendentals=0),
        compiler_params=pltpu.CompilerParams(vmem_limit_bytes=4 * 1024 * 1024),
        name="widen",
    )(edges, field, below, above)


def shards(brick_ids, voxel_offset, fractions, normals, point_weight, tile_count):
    slabs, columns = lax.axis_size("gx"), lax.axis_size("yz")
    outbox = dispatch(
        brick_ids[:, 0],
        tile_count,
        voxel_offset,
        jnp.transpose(fractions, (1, 0, 2)),
        jnp.transpose(normals, (1, 0, 2)),
        point_weight,
        slabs * columns,
    )
    inbox = lax.all_to_all(outbox, ("gx", "yz"), split_axis=0, concat_axis=0, tiled=True)
    slab, column = lax.axis_index("gx"), lax.axis_index("yz")
    edges = jnp.stack([slab, slabs - 1 - slab, column, columns - 1 - column])
    field, up, down, right, left = splat(inbox.reshape(-1, LANES))
    below = passed_along(up, "gx", 1)
    above = passed_along(down, "gx", -1)
    right, left = join(edges, below, above, right, left)
    before = passed_along(right, "yz", 1)
    after = passed_along(left, "yz", -1)
    field = widen(edges, field, below, above)
    row = lax.broadcasted_iota(jnp.int32, (1, 1, BY, 1), 2)
    first = (row == 0) & (column > 0)
    last = (row == BY - 1) & (column < columns - 1)
    before = jnp.where(first, before.reshape(2, BX, 1, BZ), 0.0)
    after = jnp.where(last, after.reshape(2, BX, 1, BZ), 0.0)
    total = field + before + after
    return total[0], total[1]


def solution(mesh):
    return jax.shard_map(
        shards,
        mesh=mesh,
        in_specs=(
            P(("gx", "yz"), None),
            P(("gx", "yz"), None),
            P(("gx", "yz"), None, None),
            P(("gx", "yz"), None, None),
            P(("gx", "yz"), None),
            P(("gx", "yz")),
        ),
        out_specs=(P("gx", "yz", None), P("gx", "yz", None)),
        check_vma=False,
    )
```

```python
import jax
import jax.numpy as jnp
from jax import lax
from jax.experimental import pallas as pl
from jax.experimental.pallas import tpu as pltpu
from jax.sharding import PartitionSpec as P

BX = 4
BY = 8
BZ = 128
CAP = 2
LANES = 128
GROUP = 8
UNROLL = 32
AHEAD = 1
SLOTS = 32
PLANES = (BX + 2) * BY
ENDS = 16
ROWS = PLANES + ENDS
ROW_X = 0
ROW_Z = 4 * (BX + 2)
ROW_COUNT = ROW_Z + 8
SIDES = 8


def passed_along(value, axis, steps):
    count = lax.axis_size(axis)
    return lax.ppermute(value, axis, [(source, (source + steps) % count) for source in range(count)])


def dispatch_kernel(ids_ref, count_ref, offset_hbm, frac_hbm, normal_hbm, weight_hbm, out_hbm, *scratch):
    offset_ref, frac_ref, normal_ref, weight_ref, out_ref, seen_ref, slot_ref, sems = scratch
    tiles, slots = ids_ref.shape[0], out_hbm.shape[0]
    pairs = ((offset_hbm, offset_ref), (frac_hbm, frac_ref), (normal_hbm, normal_ref), (weight_hbm, weight_ref))
    loads = [pltpu.make_async_copy(source, target, sems.at[i]) for i, (source, target) in enumerate(pairs)]
    for load in loads:
        load.start()

    def reset(i, _):
        seen_ref[i] = 0
        return 0

    lax.fori_loop(0, seen_ref.shape[0], reset, 0, unroll=16)

    def choose(i, _):
        for j in range(8):
            t = 8 * i + j
            brick = ids_ref[t]
            rank = seen_ref[brick]
            seen_ref[brick] = rank + 1
            slot_ref[t] = jnp.where(t < count_ref[0], brick * CAP + jnp.minimum(rank, CAP - 1), slots)
            out_ref[pl.ds(2 * t, 2)] = jnp.zeros((2,) + out_ref.shape[1:], jnp.float32)
        return 0

    lax.fori_loop(0, tiles // 8, choose, 0)
    for load in loads:
        load.wait()

    def place(i, _):
        here = pl.ds(pl.multiple_of(8 * i, 8), 8)
        rows = [frac_ref[k, here, :] for k in range(3)] + [offset_ref[here, :].astype(jnp.float32)]
        rows += [normal_ref[k, here, :] for k in range(3)] + [weight_ref[here, :]]
        for j in range(8):
            slot = slot_ref[8 * i + j]
            for half in range(out_ref.shape[1] // 8):
                for k, row in enumerate(rows):
                    piece = row[j : j + 1, LANES * half : LANES * half + LANES]
                    out_ref[slot, 8 * half + k : 8 * half + k + 1, :] = piece
        return 0

    lax.fori_loop(0, tiles // 8, place, 0)
    store = pltpu.make_async_copy(out_ref.at[pl.ds(0, slots)], out_hbm, sems.at[len(pairs)])
    store.start()
    store.wait()


def dispatch(ids, count, offset, frac, normal, weight, bricks):
    smem = pl.BlockSpec(memory_space=pltpu.SMEM)
    hbm = pl.BlockSpec(memory_space=pltpu.HBM)
    block = (8 * offset.shape[1] // LANES, LANES)
    slots = bricks * CAP
    return pl.pallas_call(
        dispatch_kernel,
        out_shape=jax.ShapeDtypeStruct((slots,) + block, jnp.float32),
        in_specs=[smem, smem, hbm, hbm, hbm, hbm],
        out_specs=hbm,
        scratch_shapes=[
            pltpu.VMEM(offset.shape, jnp.int32),
            pltpu.VMEM(frac.shape, jnp.float32),
            pltpu.VMEM(normal.shape, jnp.float32),
            pltpu.VMEM(weight.shape, jnp.float32),
            pltpu.VMEM((slots + 1,) + block, jnp.float32),
            pltpu.SMEM((bricks,), jnp.int32),
            pltpu.SMEM(ids.shape, jnp.int32),
            pltpu.SemaphoreType.DMA((5,)),
        ],
        name="dispatch",
    )(ids, count, offset, frac, normal, weight)


def spline(f):
    return (
        [0.5 * (1.0 - f) * (1.0 - f), 0.75 - (f - 0.5) * (f - 0.5), 0.5 * f * f],
        [f - 1.0, 1.0 - 2.0 * f, f],
    )


def spread(cell, cells, pieces):
    here = [cell == c for c in range(cells)]
    out = []
    for target in range(cells + 2):
        value = None
        for i in range(3):
            c = target - i
            if 0 <= c < cells:
                value = jnp.where(here[c], pieces[i], 0.0 if value is None else value)
        out.append(value)
    return out


def prepare(inbox_ref, first, row_ref, side_ref):
    def channel(c):
        return inbox_ref[pl.ds(first * 8 + c, GROUP, stride=8), :]

    def put(i, s, v):
        for h in range(2):
            side_ref[i, h, 4 * s : 4 * s + 4, :] = v[4 * h : 4 * h + 4]

    offset = channel(3).astype(jnp.int32)
    weights, slopes = spline(channel(0))
    cell = lax.shift_right_logical(offset, 10)
    x_value, x_slope = spread(cell, BX, weights), spread(cell, BX, slopes)
    weights, slopes = spline(channel(1))
    cell = lax.shift_right_logical(offset, 7) & 7
    y_value, y_slope = spread(cell, BY, weights), spread(cell, BY, slopes)
    nx, ny, nz, weight = [channel(c) for c in (4, 5, 6, 7)]
    for r in range(BX + 2):
        parts = (nx * x_slope[r], ny * x_value[r], nz * x_value[r], weight * x_value[r])
        for i, part in enumerate(parts):
            row_ref[ROW_X + 4 * r + i] = part
        for e in range(2):
            yv, ys = y_value[BY + e], y_slope[BY + e]
            ends = (parts[0] * yv + parts[1] * ys, parts[2] * yv, parts[3] * yv)
            for k in range(3):
                put(2 * k + e, r, ends[k])
    for s in range(BY):
        put(6, s, y_value[s])
        put(7, s, y_slope[s])
    weights, slopes = spline(channel(2))
    cell = offset & 127
    rows = weights + slopes + [(cell & 15).astype(jnp.float32), lax.shift_right_logical(cell, 4).astype(jnp.float32)]
    for i, row in enumerate(rows):
        row_ref[ROW_Z + i] = row


def build(row_ref, side_ref, unit):
    def row(i):
        return jnp.broadcast_to(row_ref[i, unit : unit + 1, :], (8, LANES))

    def paired(i):
        v = row(i)
        return jnp.concatenate([v, v], axis=0).astype(jnp.bfloat16)

    def side(i):
        return side_ref[i, unit // 4, pl.ds(unit % 4, 8, stride=4), :]

    y_value, y_slope = side(6), side(7)
    left = [[], [], []]
    for pair in range((BX + 2) // 2):
        blocks = []
        for r in (2 * pair, 2 * pair + 1):
            one, two, three, screen = [row(ROW_X + 4 * r + i) for i in range(4)]
            blocks.append((one * y_value + two * y_slope, three * y_value, screen * y_value))
        for k in range(3):
            left[k].append(jnp.concatenate([blocks[0][k], blocks[1][k]], axis=0).astype(jnp.bfloat16))
    for k in range(3):
        left[k].append(jnp.concatenate([side(2 * k), side(2 * k + 1)], axis=0).astype(jnp.bfloat16))

    depth = lax.broadcasted_iota(jnp.int32, (16, LANES), 0)
    zero = jnp.zeros((16, LANES), jnp.bfloat16)

    def constant(v):
        return v.astype(jnp.float32).astype(jnp.bfloat16)

    low, block_of = paired(ROW_Z + 6), paired(ROW_Z + 7)
    w = [paired(ROW_Z + i) for i in range(6)]
    below = constant((depth + 1) & 15) == low
    value, slope = jnp.where(below, w[0], zero), jnp.where(below, w[3], zero)
    carry = jnp.where(below, constant(jnp.where(depth == 15, -1, 0)), zero)
    same = constant(depth) == low
    value, slope = jnp.where(same, w[1], value), jnp.where(same, w[4], slope)
    above = constant((depth + 15) & 15) == low
    value, slope = jnp.where(above, w[2], value), jnp.where(above, w[5], slope)
    home = block_of + jnp.where(above, constant(jnp.where(depth == 0, 1, 0)), carry)
    right = [[], []]
    for block in range(BZ // 16):
        inside = home == jnp.full((16, LANES), block, jnp.bfloat16)
        right[0].append(jnp.where(inside, value, zero))
        right[1].append(jnp.where(inside, slope, zero))
    return jnp.concatenate(sum(left, []), axis=0), jnp.concatenate(sum(right, []), axis=0)


def splat_kernel(inbox_ref, field_ref, up_ref, down_ref, right_ref, left_ref, acc_ref, row_ref, side_ref):
    batch = GROUP * UNROLL
    steps = inbox_ref.shape[0] // (8 * batch)

    acc_ref[...] = jnp.zeros_like(acc_ref)

    def ready(group, slot):
        group = jnp.minimum(group, steps * UNROLL - 1)
        prepare(inbox_ref, group * GROUP, row_ref.at[slot], side_ref.at[slot])

    for u in range(AHEAD):
        ready(u, u)

    def body(i, _):
        acc = acc_ref[...]
        for u in range(UNROLL):
            slot = u % SLOTS
            for pair in range(GROUP // 2):
                sides = [build(row_ref.at[slot], side_ref.at[slot], k) for k in (2 * pair, 2 * pair + 1)]
                acc = acc + lax.dot_general(
                    jnp.concatenate([a for a, _ in sides], axis=1),
                    jnp.concatenate([z for _, z in sides], axis=1),
                    (((1,), (1,)), ((), ())),
                    preferred_element_type=jnp.float32,
                )
            ready(i * UNROLL + u + AHEAD, (u + AHEAD) % SLOTS)
        acc_ref[...] = acc
        return 0

    lax.fori_loop(0, steps, body, 0)
    for k in range(2):
        first = 2 * ROWS * k
        if k == 0:
            acc_ref[0:ROWS, 0:BZ] = acc_ref[0:ROWS, 0:BZ] + acc_ref[ROWS : 2 * ROWS, BZ : 2 * BZ]

        def rows(at, count, first=first):
            return acc_ref[first + at : first + at + count, 0:BZ]

        for r in range(BX):
            field_ref[k, r, 0 : BY - 1, :] = rows(BY * (r + 1) + 1, BY - 1)
            field_ref[k, r, BY - 1 : BY, :] = rows(PLANES + r + 1, 1)
            left_ref[BX * k + r : BX * k + r + 1, :] = rows(BY * (r + 1), 1)
        right_ref[BX * k : BX * k + BX, :] = rows(PLANES + 9, BX)
        for ref, r in ((up_ref, BX + 1), (down_ref, 0)):
            ref[BY * k : BY * k + BY - 1, :] = rows(BY * r + 1, BY - 1)
            ref[BY * k + BY - 1 : BY * k + BY, :] = rows(PLANES + r, 1)
            ref[16 + k : 17 + k, :] = rows(BY * r, 1)
            ref[18 + k : 19 + k, :] = rows(PLANES + 8 + r, 1)
    for ref in (up_ref, down_ref):
        ref[20:24, :] = jnp.zeros((4, BZ), jnp.float32)


def splat(inbox):
    vmem = pl.BlockSpec(memory_space=pltpu.VMEM)
    shapes = ((2, BX, BY, BZ), (24, BZ), (24, BZ), (2 * BX, BZ), (2 * BX, BZ))
    return pl.pallas_call(
        splat_kernel,
        out_shape=tuple(jax.ShapeDtypeStruct(shape, jnp.float32) for shape in shapes),
        in_specs=[vmem],
        out_specs=(vmem,) * len(shapes),
        scratch_shapes=[
            pltpu.VMEM((3 * ROWS, 2 * BZ), jnp.float32),
            pltpu.VMEM((SLOTS, ROW_COUNT, GROUP, LANES), jnp.float32),
            pltpu.VMEM((SLOTS, SIDES, 2, 4 * 8, LANES), jnp.float32),
        ],
        compiler_params=pltpu.CompilerParams(vmem_limit_bytes=16 * 1024 * 1024),
        name="splat",
    )(inbox)


def join_kernel(edge_ref, below_ref, above_ref, right_ref, left_ref, right_out, left_out):
    below = jnp.where(edge_ref[0] == 0, 0.0, below_ref[16:24, :])
    above = jnp.where(edge_ref[1] == 0, 0.0, above_ref[16:24, :])
    right_out[...] = right_ref[...]
    left_out[...] = left_ref[...]
    for k in range(2):
        for out, at in ((left_out, k), (right_out, 2 + k)):
            first, last = BX * k, BX * k + BX - 1
            out[first : first + 1, :] = out[first : first + 1, :] + below[at : at + 1]
            out[last : last + 1, :] = out[last : last + 1, :] + above[at : at + 1]


def join(edges, below, above, right, left):
    smem = pl.BlockSpec(memory_space=pltpu.SMEM)
    vmem = pl.BlockSpec(memory_space=pltpu.VMEM)
    shape = jax.ShapeDtypeStruct(right.shape, jnp.float32)
    return pl.pallas_call(
        join_kernel,
        out_shape=(shape, shape),
        in_specs=[smem] + [vmem] * 4,
        out_specs=(vmem, vmem),
        compiler_params=pltpu.CompilerParams(vmem_limit_bytes=4 * 1024 * 1024),
        name="join",
    )(edges, below, above, right, left)


def widen_kernel(edge_ref, field_ref, below_ref, above_ref, rhs_ref, screen_ref):
    for k, out_ref in enumerate((rhs_ref, screen_ref)):
        for r in range(BX):
            plane = field_ref[k, r]
            if r == 0:
                plane = plane + jnp.where(edge_ref[0] == 0, 0.0, below_ref[BY * k : BY * k + BY, :])
            if r == BX - 1:
                plane = plane + jnp.where(edge_ref[1] == 0, 0.0, above_ref[BY * k : BY * k + BY, :])
            out_ref[r] = plane


def widen(edges, field, below, above):
    smem = pl.BlockSpec(memory_space=pltpu.SMEM)
    vmem = pl.BlockSpec(memory_space=pltpu.VMEM)
    return pl.pallas_call(
        widen_kernel,
        out_shape=(jax.ShapeDtypeStruct(field.shape[1:], jnp.float32),) * 2,
        in_specs=[smem] + [vmem] * 3,
        out_specs=(vmem, vmem),
        cost_estimate=pl.CostEstimate(flops=20000000, bytes_accessed=100000, transcendentals=0),
        compiler_params=pltpu.CompilerParams(vmem_limit_bytes=4 * 1024 * 1024),
        name="widen",
    )(edges, field, below, above)


def shards(brick_ids, voxel_offset, fractions, normals, point_weight, tile_count):
    slabs, columns = lax.axis_size("gx"), lax.axis_size("yz")
    outbox = dispatch(
        brick_ids[:, 0],
        tile_count,
        voxel_offset,
        jnp.transpose(fractions, (1, 0, 2)),
        jnp.transpose(normals, (1, 0, 2)),
        point_weight,
        slabs * columns,
    )
    inbox = lax.all_to_all(outbox, ("gx", "yz"), split_axis=0, concat_axis=0, tiled=True)
    slab, column = lax.axis_index("gx"), lax.axis_index("yz")
    edges = jnp.stack([slab, slabs - 1 - slab, column, columns - 1 - column])
    field, up, down, right, left = splat(inbox.reshape(-1, LANES))
    below = passed_along(up, "gx", 1)
    above = passed_along(down, "gx", -1)
    right, left = join(edges, below, above, right, left)
    before = passed_along(right, "yz", 1)
    after = passed_along(left, "yz", -1)
    planes = widen(edges, field, below, above)
    row = lax.broadcasted_iota(jnp.int32, (1, BY, 1), 1)
    first = (row == 0) & (column > 0)
    last = (row == BY - 1) & (column < columns - 1)
    out = []
    for k, plane in enumerate(planes):
        part = slice(BX * k, BX * k + BX)
        out.append(plane + jnp.where(first, before[part, None], 0.0) + jnp.where(last, after[part, None], 0.0))
    return tuple(out)


def solution(mesh):
    return jax.shard_map(
        shards,
        mesh=mesh,
        in_specs=(
            P(("gx", "yz"), None),
            P(("gx", "yz"), None),
            P(("gx", "yz"), None, None),
            P(("gx", "yz"), None, None),
            P(("gx", "yz"), None),
            P(("gx", "yz")),
        ),
        out_specs=(P("gx", "yz", None), P("gx", "yz", None)),
        check_vma=False,
    )
```
